8 devices in a mesh: dp: 1 (over z), tp: 8 (over y, x, core).
Axes of the slice: x: 2, y: 2, z: 1, core: 2. Of those that a mesh axis runs over, the one named last changes fastest.
Arguments:
- tokens: bfloat16 [4, 4096, 1152], P('dp', 'tp')
- ln1_gain: float32 [1152], replicated
- ln1_bias: float32 [1152], replicated
- w_qkv: bfloat16 [1152, 3, 16, 72], P(None, None, 'tp')
- b_qkv: float32 [3, 16, 72], P(None, 'tp')
- w_out: bfloat16 [16, 72, 1152], P('tp')
- b_out: float32 [1152], replicated
- ln2_gain: float32 [1152], replicated
- ln2_bias: float32 [1152], replicated
- w_up: bfloat16 [1152, 4304], P(None, 'tp')
- b_up: float32 [4304], P('tp')
- w_down: bfloat16 [4304, 1152], P('tp')
- b_down: float32 [1152], replicated
- lnf_gain: float32 [1152], replicated
- lnf_bias: float32 [1152], replicated
- probe_vec: bfloat16 [1152], replicated
- map_wq: bfloat16 [1152, 16, 72], replicated
- map_bq: float32 [16, 72], replicated
- map_wkv: bfloat16 [1152, 2, 16, 72], replicated
- map_bkv: float32 [2, 16, 72], replicated
- map_wo: bfloat16 [16, 72, 1152], replicated
- map_bo: float32 [1152], replicated
- map_ln_gain: float32 [1152], replicated
- map_ln_bias: float32 [1152], replicated
- map_w_up: bfloat16 [1152, 4304], replicated
- map_b_up: float32 [4304], replicated
- map_w_down: bfloat16 [4304, 1152], replicated
- map_b_down: float32 [1152], replicated
Outputs:
- output: bfloat16 [4, 1152], P('dp')
All inputs are finite; a program needn't handle non-finite values.
Results may differ from the reference program's by a relative error of at most 0.0105538.
Values are sent between devices in bfloat16 or wider.
A program may use at most 1 GiB of HBM per device.

```python
import math
import jax
import jax.numpy as jnp
from jax import lax

BATCH_SIZE = 4
SEQ_LEN = 4096
MODEL_DIM = 1152
NUM_HEADS = 16
HEAD_DIM = 72
MLP_DIM = 4304
LN_EPS = 1e-6


def normal_draw(rng_key, arr_shape, std_dev):
    return jax.random.normal(rng_key, arr_shape, jnp.float32) * std_dev


def weight_draw(rng_key, arr_shape, fan_in):
    return normal_draw(rng_key, arr_shape, fan_in ** -0.5).astype(jnp.bfloat16)


def setup_inputs(seed: int = 0, part: int = 0) -> dict:
    part_key = jax.random.fold_in(jax.random.key(seed), part)
    noise_key, spread_key = jax.random.split(part_key)
    shared_keys = jax.random.split(jax.random.key(seed + 1), 27)
    probe_scale = math.sqrt(0.5 * math.log(SEQ_LEN / 8))
    qkv_scale = jnp.array([probe_scale, 1.0, 1.0], jnp.float32)[:, None, None]
    token_scale = jnp.exp(0.5 * jax.random.normal(spread_key, (BATCH_SIZE, SEQ_LEN, 1), jnp.float32))
    tokens = normal_draw(noise_key, (BATCH_SIZE, SEQ_LEN, MODEL_DIM), 1.0) * token_scale
    w_qkv = normal_draw(shared_keys[2], (MODEL_DIM, 3, NUM_HEADS, HEAD_DIM), MODEL_DIM ** -0.5) * qkv_scale
    return {
        'tokens': tokens.astype(jnp.bfloat16),
        'ln1_gain': 1.0 + normal_draw(shared_keys[0], (MODEL_DIM,), 0.8),
        'ln1_bias': normal_draw(shared_keys[1], (MODEL_DIM,), 0.3),
        'w_qkv': w_qkv.astype(jnp.bfloat16),
        'b_qkv': normal_draw(shared_keys[3], (3, NUM_HEADS, HEAD_DIM), 0.5),
        'w_out': weight_draw(shared_keys[4], (NUM_HEADS, HEAD_DIM, MODEL_DIM), MODEL_DIM),
        'b_out': normal_draw(shared_keys[5], (MODEL_DIM,), 0.5),
        'ln2_gain': 1.0 + normal_draw(shared_keys[6], (MODEL_DIM,), 0.3),
        'ln2_bias': normal_draw(shared_keys[7], (MODEL_DIM,), 0.3),
        'w_up': weight_draw(shared_keys[8], (MODEL_DIM, MLP_DIM), MODEL_DIM),
        'b_up': normal_draw(shared_keys[9], (MLP_DIM,), 0.5),
        'w_down': weight_draw(shared_keys[10], (MLP_DIM, MODEL_DIM), MLP_DIM),
        'b_down': normal_draw(shared_keys[11], (MODEL_DIM,), 0.5),
        'lnf_gain': 1.0 + normal_draw(shared_keys[12], (MODEL_DIM,), 0.3),
        'lnf_bias': normal_draw(shared_keys[13], (MODEL_DIM,), 0.3),
        'probe_vec': normal_draw(shared_keys[14], (MODEL_DIM,), probe_scale).astype(jnp.bfloat16),
        'map_wq': weight_draw(shared_keys[15], (MODEL_DIM, NUM_HEADS, HEAD_DIM), MODEL_DIM),
        'map_bq': normal_draw(shared_keys[16], (NUM_HEADS, HEAD_DIM), probe_scale),
        'map_wkv': weight_draw(shared_keys[17], (MODEL_DIM, 2, NUM_HEADS, HEAD_DIM), MODEL_DIM),
        'map_bkv': normal_draw(shared_keys[18], (2, NUM_HEADS, HEAD_DIM), 0.5),
        'map_wo': weight_draw(shared_keys[19], (NUM_HEADS, HEAD_DIM, MODEL_DIM), MODEL_DIM),
        'map_bo': normal_draw(shared_keys[20], (MODEL_DIM,), 0.5),
        'map_ln_gain': 1.0 + normal_draw(shared_keys[21], (MODEL_DIM,), 0.3),
        'map_ln_bias': normal_draw(shared_keys[22], (MODEL_DIM,), 0.3),
        'map_w_up': weight_draw(shared_keys[23], (MODEL_DIM, MLP_DIM), MODEL_DIM),
        'map_b_up': normal_draw(shared_keys[24], (MLP_DIM,), 0.5),
        'map_w_down': weight_draw(shared_keys[25], (MLP_DIM, MODEL_DIM), MLP_DIM),
        'map_b_down': normal_draw(shared_keys[26], (MODEL_DIM,), 0.5),
    }


def layer_norm(values, gain_vec, bias_vec):
    centered = values - jnp.mean(values, axis=-1, keepdims=True)
    variance = jnp.mean(centered * centered, axis=-1, keepdims=True)
    return centered * lax.rsqrt(variance + LN_EPS) * gain_vec + bias_vec


def project(activations, weight, bias_arr):
    return (jnp.einsum('bnd,dhe->bnhe', activations.astype(jnp.float32), weight.astype(jnp.float32)) + bias_arr).astype(jnp.bfloat16)


def head_attention(query_h, key_h, value_h):
    scores = jnp.dot(query_h, key_h.T, preferred_element_type=jnp.float32) * HEAD_DIM ** -0.5
    weights = jnp.exp(scores - jnp.max(scores, axis=-1, keepdims=True))
    weight_sum = jnp.sum(weights, axis=-1, keepdims=True)
    mixed_vals = jnp.dot(weights.astype(jnp.bfloat16), value_h, preferred_element_type=jnp.float32)
    return (mixed_vals / weight_sum).astype(jnp.bfloat16)


def batch_attention(batch_trio):
    return lax.map(lambda head_trio: head_attention(head_trio[0], head_trio[1], head_trio[2]), batch_trio)


def reference(tokens, ln1_gain, ln1_bias, w_qkv, b_qkv, w_out, b_out, ln2_gain, ln2_bias, w_up, b_up, w_down, b_down, lnf_gain, lnf_bias, probe_vec, map_wq, map_bq, map_wkv, map_bkv, map_wo, map_bo, map_ln_gain, map_ln_bias, map_w_up, map_b_up, map_w_down, map_b_down):
    hidden = layer_norm(tokens.astype(jnp.float32), ln1_gain, ln1_bias).astype(jnp.bfloat16)
    per_head = tuple(jnp.transpose(project(hidden, w_qkv[:, qkv_index], b_qkv[qkv_index]), (0, 2, 1, 3)) for qkv_index in range(3))
    attended = lax.map(batch_attention, per_head)
    attn_out = jnp.einsum('bhne,hed->bnd', attended.astype(jnp.float32), w_out.astype(jnp.float32)) + b_out
    resid_one = (tokens.astype(jnp.float32) + attn_out).astype(jnp.bfloat16)
    hidden_two = layer_norm(resid_one.astype(jnp.float32), ln2_gain, ln2_bias).astype(jnp.bfloat16)
    pre_act = jnp.einsum('bnd,df->bnf', hidden_two.astype(jnp.float32), w_up.astype(jnp.float32)) + b_up
    activated = jax.nn.gelu(pre_act, approximate=True).astype(jnp.bfloat16)
    mlp_out = jnp.einsum('bnf,fd->bnd', activated.astype(jnp.float32), w_down.astype(jnp.float32)) + b_down
    resid_two = (resid_one.astype(jnp.float32) + mlp_out).astype(jnp.bfloat16)
    encoded = layer_norm(resid_two.astype(jnp.float32), lnf_gain, lnf_bias).astype(jnp.bfloat16)
    probe_q = (jnp.einsum('d,dhe->he', probe_vec.astype(jnp.float32), map_wq.astype(jnp.float32)) + map_bq).astype(jnp.bfloat16)
    map_keys = project(encoded, map_wkv[:, 0], map_bkv[0])
    map_vals = project(encoded, map_wkv[:, 1], map_bkv[1])
    map_scores = jnp.einsum('he,bnhe->bhn', probe_q.astype(jnp.float32), map_keys.astype(jnp.float32)) * HEAD_DIM ** -0.5
    map_weights = jnp.exp(map_scores - jnp.max(map_scores, axis=-1, keepdims=True))
    map_sum = jnp.sum(map_weights, axis=-1, keepdims=True)
    mixed_heads = jnp.einsum('bhn,bnhe->bhe', map_weights.astype(jnp.bfloat16).astype(jnp.float32), map_vals.astype(jnp.float32))
    pooled_heads = (mixed_heads / map_sum).astype(jnp.bfloat16)
    attn_vec = jnp.einsum('bhe,hed->bd', pooled_heads.astype(jnp.float32), map_wo.astype(jnp.float32)) + map_bo
    map_hidden = layer_norm(attn_vec, map_ln_gain, map_ln_bias).astype(jnp.bfloat16)
    map_act = jax.nn.gelu(jnp.dot(map_hidden, map_w_up, preferred_element_type=jnp.float32) + map_b_up, approximate=True).astype(jnp.bfloat16)
    return (attn_vec + jnp.dot(map_act, map_w_down, preferred_element_type=jnp.float32) + map_b_down).astype(jnp.bfloat16)
```

```python
import functools

import jax
import jax.numpy as jnp
from jax import lax
from jax.experimental import pallas as pl
from jax.experimental.pallas import tpu as pltpu
from jax.sharding import PartitionSpec as P

LN_EPS = 1e-6
LOG2E = 1.4426950408889634
LANES = 128


def layer_norm(values, gain_vec, bias_vec):
    centered = values - jnp.mean(values, axis=-1, keepdims=True)
    variance = jnp.mean(centered * centered, axis=-1, keepdims=True)
    return centered * lax.rsqrt(variance + LN_EPS) * gain_vec + bias_vec


def round_up(size, multiple):
    return -(-size // multiple) * multiple


def attention_kernel(head_dim, chunk, q_ref, k_ref, v_ref, out_ref, scores_a, scores_b, max_a, max_b, first_out):
    n_keys = k_ref.shape[0]
    block = q_ref.shape[1]
    n_chunks = n_keys // chunk
    exp_scale = head_dim ** -0.5 * LOG2E

    def score_chunk(head, index, scores, running):
        rows = pl.ds(index * chunk, chunk)
        keys = k_ref[rows, head * LANES:(head + 1) * LANES]
        part = jnp.dot(keys, q_ref[head * LANES:(head + 1) * LANES, :], preferred_element_type=jnp.float32)
        scores[rows, :] = part
        part_max = jnp.max(part.reshape(chunk // 8, 8, block), axis=0)
        return part_max if running is None else jnp.maximum(running, part_max)

    def mix_chunk(head, index, scores, peak, total, mixed):
        rows = pl.ds(index * chunk, chunk)
        weights = jnp.exp2((scores[rows, :] - peak) * exp_scale)
        part_total = jnp.sum(weights.reshape(chunk // 8, 8, block), axis=0)
        values = v_ref[head * v_rows:(head + 1) * v_rows, index * chunk:(index + 1) * chunk]
        part_mixed = jnp.dot(values, weights.astype(jnp.bfloat16), preferred_element_type=jnp.float32)
        if total is None:
            return part_total, part_mixed
        return total + part_total, mixed + part_mixed

    v_rows = v_ref.shape[0] // 2

    def overlap(score_head, score_buf, max_buf, mix_head, mix_buf, mix_max):
        running, total, mixed = None, None, None
        peak = jnp.max(mix_max[...], axis=0, keepdims=True)
        for index in range(n_chunks):
            running = score_chunk(score_head, index, score_buf, running)
            total, mixed = mix_chunk(mix_head, index, mix_buf, peak, total, mixed)
        max_buf[...] = running
        return mixed[:head_dim] / jnp.sum(total, axis=0, keepdims=True)

    @pl.when(pl.program_id(0) == 0)
    def _():
        scores_b[...] = jnp.zeros_like(scores_b)
        max_b[...] = jnp.zeros_like(max_b)
        first_out[...] = jnp.zeros_like(first_out)

    second = overlap(0, scores_a, max_a, 1, scores_b, max_b)
    out_ref[0] = jnp.concatenate([first_out[...], second], axis=0).astype(out_ref.dtype)
    first_out[...] = overlap(1, scores_b, max_b, 0, scores_a, max_a)


def image_attention(queries_t, keys, values_t, head_dim, n_blocks):
    n_keys = keys.shape[0]
    block = n_keys // n_blocks
    flops = 2 * 2 * n_keys * n_keys * 2 * LANES
    return pl.pallas_call(
        functools.partial(attention_kernel, head_dim, 256),
        grid=(n_blocks + 1,),
        out_shape=jax.ShapeDtypeStruct((n_blocks, 2 * head_dim, block), jnp.bfloat16),
        in_specs=[
            pl.BlockSpec((queries_t.shape[0], block), lambda i: (0, jnp.minimum(i, n_blocks - 1))),
            pl.BlockSpec(keys.shape, lambda i: (0, 0)),
            pl.BlockSpec(values_t.shape, lambda i: (0, 0)),
        ],
        out_specs=pl.BlockSpec((1, 2 * head_dim, block), lambda i: (jnp.maximum(i - 1, 0), 0, 0)),
        scratch_shapes=[
            pltpu.VMEM((n_keys, block), jnp.float32),
            pltpu.VMEM((n_keys, block), jnp.float32),
            pltpu.VMEM((8, block), jnp.float32),
            pltpu.VMEM((8, block), jnp.float32),
            pltpu.VMEM((head_dim, block), jnp.float32),
        ],
        compiler_params=pltpu.CompilerParams(dimension_semantics=('arbitrary',), vmem_limit_bytes=44 * 1024 * 1024),
        cost_estimate=pl.CostEstimate(flops=flops, bytes_accessed=8 * 1024 * 1024, transcendentals=2 * n_keys * n_keys),
        name='image_attention',
    )(queries_t, keys, values_t)


def map_tail(pooled_heads, map_wo, map_bo, map_ln_gain, map_ln_bias, map_w_up, map_b_up, map_w_down, map_b_down):
    attn_vec = jnp.einsum('bhe,hed->bd', pooled_heads, map_wo, preferred_element_type=jnp.float32) + map_bo
    map_hidden = layer_norm(attn_vec, map_ln_gain, map_ln_bias).astype(jnp.bfloat16)
    map_act = jax.nn.gelu(jnp.dot(map_hidden, map_w_up, preferred_element_type=jnp.float32) + map_b_up, approximate=True).astype(jnp.bfloat16)
    return (attn_vec + jnp.dot(map_act, map_w_down, preferred_element_type=jnp.float32) + map_b_down).astype(jnp.bfloat16)


def solution(mesh):
    tp_size = mesh.shape['tp']
    in_specs = (P('dp', 'tp', None), P(), P(), P(None, None, 'tp', None), P(None, 'tp', None), P('tp', None, None), P(), P(), P(), P(None, 'tp'), P('tp'), P('tp', None)) + (P(),) * 16

    def local_program(tokens, ln1_gain, ln1_bias, w_qkv, b_qkv, w_out, b_out, ln2_gain, ln2_bias, w_up, b_up, w_down, b_down, lnf_gain, lnf_bias, probe_vec, map_wq, map_bq, map_wkv, map_bkv, map_wo, map_bo, map_ln_gain, map_ln_bias, map_w_up, map_b_up, map_w_down, map_b_down):
        n_images, run, width = tokens.shape
        n_heads, head_dim = w_qkv.shape[2:]
        hidden_units = w_up.shape[1]

        gathered = []
        for image in range(n_images):
            hidden = layer_norm(tokens[image].astype(jnp.float32), ln1_gain, ln1_bias).astype(jnp.bfloat16)
            gathered.append(lax.all_gather(hidden, 'tp', axis=0, tiled=True))

        v_rows = round_up(head_dim, 16)
        wk = jnp.pad(w_qkv[:, 1], ((0, 0), (0, 0), (0, LANES - head_dim))).reshape(width, n_heads * LANES)
        bk = jnp.pad(b_qkv[1], ((0, 0), (0, LANES - head_dim))).reshape(n_heads * LANES)
        wq_t = jnp.pad(jnp.transpose(w_qkv[:, 0], (1, 2, 0)), ((0, 0), (0, LANES - head_dim), (0, 0))).reshape(n_heads * LANES, width)
        bq = jnp.pad(b_qkv[0], ((0, 0), (0, LANES - head_dim))).reshape(n_heads * LANES, 1)
        wv_t = jnp.pad(jnp.transpose(w_qkv[:, 2], (1, 2, 0)), ((0, 0), (0, v_rows - head_dim), (0, 0))).reshape(n_heads * v_rows, width)
        bv = jnp.pad(b_qkv[2], ((0, 0), (0, v_rows - head_dim))).reshape(n_heads * v_rows, 1)

        padded = round_up(hidden_units, 32)
        w_up_t = jnp.pad(w_up.T, ((0, padded - hidden_units), (0, 0)))
        w_down_p = jnp.pad(w_down, ((0, padded - hidden_units), (0, 0)))
        b_up_all = lax.all_gather(jnp.pad(b_up, (0, padded - hidden_units)), 'tp', axis=0, tiled=True)
        w_out_all = lax.all_gather(w_out.reshape(n_heads * head_dim, width), 'tp', axis=0, tiled=True)
        w_up_all = lax.all_gather(w_up_t, 'tp', axis=0, tiled=True)
        w_down_all = lax.all_gather(w_down_p, 'tp', axis=0, tiled=True)

        def swap(mixed):
            return lax.all_to_all(mixed, 'tp', split_axis=0, concat_axis=0, tiled=True).reshape(tp_size * n_heads * head_dim, run)

        exchanged = []
        for image in range(n_images):
            h_all = gathered[image]
            if exchanged:
                h_all, mixed = lax.optimization_barrier((h_all, mixed))
                exchanged[-1] = swap(mixed)
            keys = (jnp.dot(h_all, wk, preferred_element_type=jnp.float32) + bk).astype(jnp.bfloat16)
            queries_t = (lax.dot_general(wq_t, h_all, (((1,), (1,)), ((), ())), preferred_element_type=jnp.float32) + bq).astype(jnp.bfloat16)
            values_t = (lax.dot_general(wv_t, h_all, (((1,), (1,)), ((), ())), preferred_element_type=jnp.float32) + bv).astype(jnp.bfloat16)
            mixed = image_attention(queries_t, keys, values_t, head_dim, tp_size)
            exchanged.append(swap(mixed))

        def finish(images):
            outs = []
            for image in images:
                attn_local = lax.dot_general(exchanged[image], w_out_all, (((0,), (0,)), ((), ())), preferred_element_type=jnp.float32)
                outs.append((tokens[image].astype(jnp.float32) + attn_local + b_out).astype(jnp.bfloat16))
            resid_one = jnp.concatenate(outs, axis=0)
            hidden_two = layer_norm(resid_one.astype(jnp.float32), ln2_gain, ln2_bias).astype(jnp.bfloat16)
            pre_act = lax.dot_general(hidden_two, w_up_all, (((1,), (1,)), ((), ())), preferred_element_type=jnp.float32) + b_up_all
            activated = jax.nn.gelu(pre_act, approximate=True).astype(jnp.bfloat16)
            mlp_local = jnp.dot(activated, w_down_all, preferred_element_type=jnp.float32)
            resid_two = (resid_one.astype(jnp.float32) + mlp_local + b_down).astype(jnp.bfloat16)
            return layer_norm(resid_two.astype(jnp.float32), lnf_gain, lnf_bias).astype(jnp.bfloat16)

        encoded = jnp.concatenate([finish(range(n_images - 1)), finish([n_images - 1])], axis=0)

        probe_q = (jnp.einsum('d,dhe->he', probe_vec, map_wq, preferred_element_type=jnp.float32) + map_bq).astype(jnp.bfloat16)
        kv_local = (jnp.einsum('nd,dthe->nthe', encoded, map_wkv, preferred_element_type=jnp.float32) + map_bkv).astype(jnp.bfloat16)
        kv_local = kv_local.reshape(n_images, run, *kv_local.shape[1:])
        scores = jnp.einsum('he,bnhe->bhn', probe_q, kv_local[:, :, 0], preferred_element_type=jnp.float32) * head_dim ** -0.5
        peak = jnp.max(scores, axis=-1, keepdims=True)
        weights = jnp.exp(scores - peak)
        total = jnp.sum(weights, axis=-1, keepdims=True)
        mixed = jnp.einsum('bhn,bnhe->bhe', weights.astype(jnp.bfloat16), kv_local[:, :, 1], preferred_element_type=jnp.float32)
        parts = lax.all_gather(jnp.concatenate([mixed, total, peak], axis=-1), 'tp', axis=0, tiled=False)
        mixed_all, total_all, peak_all = parts[..., :head_dim], parts[..., head_dim:head_dim + 1], parts[..., head_dim + 1:]
        share = jnp.exp(peak_all - jnp.max(peak_all, axis=0, keepdims=True))
        pooled_heads = (jnp.sum(mixed_all * share, axis=0) / jnp.sum(total_all * share, axis=0)).astype(jnp.bfloat16)
        return map_tail(pooled_heads, map_wo, map_bo, map_ln_gain, map_ln_bias, map_w_up, map_b_up, map_w_down, map_b_down)

    return jax.shard_map(local_program, mesh=mesh, in_specs=in_specs, out_specs=P('dp', None), check_vma=False)
```

```python
import functools

import jax
import jax.numpy as jnp
from jax import lax
from jax.experimental import pallas as pl
from jax.experimental.layout import Layout, with_layout_constraint
from jax.experimental.pallas import tpu as pltpu
from jax.sharding import PartitionSpec as P

LN_EPS = 1e-6
LOG2E = 1.4426950408889634
LANES = 128


def layer_norm(values, gain_vec, bias_vec):
    centered = values - jnp.mean(values, axis=-1, keepdims=True)
    variance = jnp.mean(centered * centered, axis=-1, keepdims=True)
    return centered * lax.rsqrt(variance + LN_EPS) * gain_vec + bias_vec


def row_major(values):
    return with_layout_constraint(values, Layout(major_to_minor=tuple(range(values.ndim))))


def round_up(size, multiple):
    return -(-size // multiple) * multiple


def attention_kernel(head_dim, chunk, q_ref, k_own_ref, k_far_ref, v_own_ref, v_far_ref, v_own_last_ref, v_far_last_ref, *refs):
    out_ref, scores_a, scores_b, max_a, max_b, first_out = refs[-6:]
    half_keys = k_own_ref.shape[1]
    block = q_ref.shape[1] // 2
    step = pl.program_id(0)
    exp_scale = head_dim ** -0.5 * LOG2E

    def score_chunk(keys_t, queries, rows, scores, running):
        part = lax.dot_general(keys_t, queries, (((0,), (0,)), ((), ())), preferred_element_type=jnp.float32)
        scores[rows, :] = part
        part_max = jnp.max(part.reshape(chunk // 8, 8, block), axis=0)
        return part_max if running is None else jnp.maximum(running, part_max)

    def mix_chunk(values, rows, scores, peak, total, mixed):
        weights = jnp.exp2((scores[rows, :] - peak) * exp_scale)
        part_total = jnp.sum(weights.reshape(chunk // 8, 8, block), axis=0)
        part_mixed = jnp.dot(values, weights.astype(jnp.bfloat16), preferred_element_type=jnp.float32)
        if total is None:
            return part_total, part_mixed
        return total + part_total, mixed + part_mixed

    def overlap(query_slot, score_buf, max_buf, v_own, v_far, mix_buf, mix_max):
        running, total, mixed = None, None, None
        peak = jnp.max(mix_max[...], axis=0, keepdims=True)
        queries = q_ref[:, query_slot * block:(query_slot + 1) * block]
        for half, (k_ref, v_ref) in enumerate(((k_own_ref, v_own), (k_far_ref, v_far))):
            for start in range(0, half_keys, chunk):
                rows = pl.ds(half * half_keys + start, chunk)
                running = score_chunk(k_ref[:, start:start + chunk], queries, rows, score_buf, running)
                total, mixed = mix_chunk(v_ref[:, start:start + chunk], rows, mix_buf, peak, total, mixed)
        max_buf[...] = running
        return mixed / jnp.sum(total, axis=0, keepdims=True)

    def write(rows, values_t):
        filled = jnp.concatenate([values_t, jnp.zeros((LANES - head_dim, block), jnp.float32)], axis=0)
        out_ref[rows, :] = filled.T.astype(out_ref.dtype)

    @pl.when(step == 0)
    def _():
        scores_b[...] = jnp.zeros_like(scores_b)
        max_b[...] = jnp.zeros_like(max_b)
        first_out[...] = jnp.zeros_like(first_out)

    @pl.when(step >= 0)
    def _():
        second = overlap(0, scores_a, max_a, v_own_last_ref, v_far_last_ref, scores_b, max_b)
        write(slice(0, block), first_out[...])
        write(slice(block, 2 * block), second)

    @pl.when(step >= 0)
    def _():
        first_out[...] = overlap(1, scores_b, max_b, v_own_ref, v_far_ref, scores_a, max_a)


def heads_attention(qkv_own, qkv_far, head_dim, heads, place, stride, previous, n_out):
    first, count = heads
    n_own = qkv_own.shape[1]
    pair = n_own // 2
    per_head = n_own // pair
    last = count * per_head - 1
    now = lambda i: first + jnp.minimum(i, last) // per_head
    before = lambda i: first + jnp.maximum(i - 1, 0) // per_head
    whole = (head_dim, n_own)
    in_specs = [
        pl.BlockSpec((head_dim, pair), lambda i: (3 * now(i), jnp.minimum(i, last) % per_head)),
        pl.BlockSpec(whole, lambda i: (3 * now(i) + 1, 0)),
        pl.BlockSpec(whole, lambda i: (3 * now(i) + 1, 0)),
        pl.BlockSpec(whole, lambda i: (3 * now(i) + 2, 0)),
        pl.BlockSpec(whole, lambda i: (3 * now(i) + 2, 0)),
        pl.BlockSpec(whole, lambda i: (3 * before(i) + 2, 0)),
        pl.BlockSpec(whole, lambda i: (3 * before(i) + 2, 0)),
    ]
    operands = [qkv_own, qkv_own, qkv_far, qkv_own, qkv_far, qkv_own, qkv_far]
    aliases = {}
    if previous is not None:
        in_specs.append(pl.BlockSpec(memory_space=pl.ANY))
        operands.append(previous)
        aliases = {7: 0}
    scored = count * n_own * 2 * n_own
    return pl.pallas_call(
        functools.partial(attention_kernel, head_dim, 256),
        grid=(last + 2,),
        out_shape=jax.ShapeDtypeStruct((n_own, n_out * LANES), jnp.bfloat16),
        in_specs=in_specs,
        out_specs=pl.BlockSpec((pair, LANES), lambda i: (jnp.maximum(i - 1, 0) % per_head, place + stride * before(i))),
        scratch_shapes=[
            pltpu.VMEM((2 * n_own, pair // 2), jnp.float32),
            pltpu.VMEM((2 * n_own, pair // 2), jnp.float32),
            pltpu.VMEM((8, pair // 2), jnp.float32),
            pltpu.VMEM((8, pair // 2), jnp.float32),
            pltpu.VMEM((head_dim, pair // 2), jnp.float32),
        ],
        input_output_aliases=aliases,
        compiler_params=pltpu.CompilerParams(dimension_semantics=('arbitrary',), vmem_limit_bytes=40 * 1024 * 1024),
        cost_estimate=pl.CostEstimate(flops=4 * scored * LANES, bytes_accessed=8 * 1024 * 1024, transcendentals=scored),
        name='heads_attention',
    )(*operands)


def map_tail(pooled_heads, map_wo, map_bo, map_ln_gain, map_ln_bias, map_w_up, map_b_up, map_w_down, map_b_down):
    attn_vec = jnp.einsum('bhe,hed->bd', pooled_heads, map_wo, preferred_element_type=jnp.float32) + map_bo
    map_hidden = layer_norm(attn_vec, map_ln_gain, map_ln_bias).astype(jnp.bfloat16)
    map_act = jax.nn.gelu(jnp.dot(map_hidden, map_w_up, preferred_element_type=jnp.float32) + map_b_up, approximate=True).astype(jnp.bfloat16)
    return (attn_vec + jnp.dot(map_act, map_w_down, preferred_element_type=jnp.float32) + map_b_down).astype(jnp.bfloat16)


def solution(mesh):
    tp_size = mesh.shape['tp']
    in_specs = (P('dp', 'tp', None), P(), P(), P(None, None, 'tp', None), P(None, 'tp', None), P('tp', None, None), P(), P(), P(), P(None, 'tp'), P('tp'), P('tp', None)) + (P(),) * 16
    partner = [(device, device ^ 1) for device in range(tp_size)]

    def local_program(tokens, ln1_gain, ln1_bias, w_qkv, b_qkv, w_out, b_out, ln2_gain, ln2_bias, w_up, b_up, w_down, b_down, lnf_gain, lnf_bias, probe_vec, map_wq, map_bq, map_wkv, map_bkv, map_wo, map_bo, map_ln_gain, map_ln_bias, map_w_up, map_b_up, map_w_down, map_b_down):
        n_images, run, width = tokens.shape
        groups, head_dim = w_qkv.shape[2:]
        n_heads = groups * tp_size
        hidden_units = w_up.shape[1]
        own = n_images * run

        resid = row_major(lax.all_to_all(row_major(tokens.reshape(tp_size, own // tp_size, width)), 'tp', split_axis=0, concat_axis=0, tiled=True).reshape(own, width))

        shards = [jnp.transpose(w_qkv[:, :, group], (1, 2, 0)).reshape(3 * head_dim, width) for group in range(groups)]
        padded = round_up(hidden_units, 32)
        w_up_t = jnp.pad(w_up.T, ((0, padded - hidden_units), (0, 0)))
        w_down_p = jnp.pad(w_down, ((0, padded - hidden_units), (0, 0)))
        biases = jnp.concatenate([b_qkv.reshape(-1), b_up])
        biases = jnp.pad(biases, (0, -biases.shape[0] % (8 * LANES))).reshape(8, -1)
        biases = lax.all_gather(biases, 'tp', axis=0, tiled=False).reshape(tp_size, -1)
        b_qkv_all = biases[:, :3 * groups * head_dim].reshape(tp_size, 3, groups, head_dim)
        b_up_all = jnp.pad(biases[:, 3 * groups * head_dim:][:, :hidden_units], ((0, 0), (0, padded - hidden_units))).reshape(tp_size * padded)

        gathered = [lax.all_gather(shards[0], 'tp', axis=0, tiled=True)]
        resid, later, w_out, w_up_t, w_down_p = lax.optimization_barrier((resid, shards[1:], w_out, w_up_t, w_down_p))
        gathered += [lax.all_gather(shard, 'tp', axis=0, tiled=True) for shard in later]
        w_out_all = lax.all_gather(w_out.reshape(groups * head_dim, width), 'tp', axis=0, tiled=True)
        w_up_all = lax.all_gather(w_up_t, 'tp', axis=0, tiled=True)
        w_down_all = lax.all_gather(w_down_p, 'tp', axis=0, tiled=True)

        hidden = row_major(layer_norm(resid.astype(jnp.float32), ln1_gain, ln1_bias).astype(jnp.bfloat16))

        def projections(group, hidden):
            product = lax.dot_general(gathered[group], hidden, (((1,), (1,)), ((), ())), preferred_element_type=jnp.float32)
            qkv_t = (product + b_qkv_all[:, :, group].reshape(-1, 1)).astype(jnp.bfloat16)
            return qkv_t, lax.ppermute(qkv_t, 'tp', partner)

        half = tp_size // 2
        first_group = projections(0, hidden)
        mixed = heads_attention(*first_group, head_dim, (0, half), 0, groups, None, n_heads)
        mixed, hidden_later = lax.optimization_barrier((mixed, hidden))
        second_group = projections(1, hidden_later)
        mixed = heads_attention(*first_group, head_dim, (half, half), 0, groups, mixed, n_heads)
        mixed = heads_attention(*second_group, head_dim, (0, tp_size), 1, groups, mixed, n_heads)

        w_out_rows = jnp.pad(w_out_all.reshape(n_heads, head_dim, width), ((0, 0), (0, LANES - head_dim), (0, 0))).reshape(n_heads * LANES, width)
        attn_local = jnp.dot(mixed, w_out_rows, preferred_element_type=jnp.float32)
        resid_one = row_major((resid.astype(jnp.float32) + attn_local + b_out).astype(jnp.bfloat16))
        hidden_two = layer_norm(resid_one.astype(jnp.float32), ln2_gain, ln2_bias).astype(jnp.bfloat16)
        pre_act = lax.dot_general(hidden_two, w_up_all, (((1,), (1,)), ((), ())), preferred_element_type=jnp.float32) + b_up_all
        activated = jax.nn.gelu(pre_act, approximate=True).astype(jnp.bfloat16)
        mlp_local = jnp.dot(activated, w_down_all, preferred_element_type=jnp.float32)
        resid_two = row_major((resid_one.astype(jnp.float32) + mlp_local + b_down).astype(jnp.bfloat16))
        encoded = layer_norm(resid_two.astype(jnp.float32), lnf_gain, lnf_bias).astype(jnp.bfloat16)

        probe_q = (jnp.dot(probe_vec[None], map_wq.reshape(width, width), preferred_element_type=jnp.float32)[0] + map_bq.reshape(width)).astype(jnp.bfloat16)
        head_of = jnp.arange(width) // head_dim
        on_head = head_of[:, None] == jnp.arange(n_heads)[None]
        probe_cols = jnp.where(on_head, probe_q[:, None], jnp.zeros((), jnp.bfloat16))
        map_keys = (jnp.dot(encoded, map_wkv[:, 0].reshape(width, width), preferred_element_type=jnp.float32) + map_bkv[0].reshape(width)).astype(jnp.bfloat16)
        map_vals = (jnp.dot(encoded, map_wkv[:, 1].reshape(width, width), preferred_element_type=jnp.float32) + map_bkv[1].reshape(width)).astype(jnp.bfloat16)
        scores = lax.dot_general(probe_cols, map_keys, (((0,), (1,)), ((), ())), preferred_element_type=jnp.float32) * head_dim ** -0.5
        peak = jnp.max(scores, axis=-1, keepdims=True)
        weights = jnp.exp(scores - peak)
        total = jnp.sum(weights, axis=-1, keepdims=True)
        every_head = jnp.dot(weights.astype(jnp.bfloat16), map_vals, preferred_element_type=jnp.float32)
        pooled = jnp.sum(jnp.where(on_head.T, every_head, 0.0).reshape(n_heads, n_heads, head_dim), axis=1)
        parts = lax.all_gather(jnp.concatenate([pooled, total, peak], axis=-1), 'tp', axis=0, tiled=False)
        parts = parts.reshape(n_images, tp_size // n_images, n_heads, head_dim + 2)
        pooled_all, total_all, peak_all = parts[..., :head_dim], parts[..., head_dim:head_dim + 1], parts[..., head_dim + 1:]
        share = jnp.exp(peak_all - jnp.max(peak_all, axis=1, keepdims=True))
        pooled_heads = (jnp.sum(pooled_all * share, axis=1) / jnp.sum(total_all * share, axis=1)).astype(jnp.bfloat16)
        return map_tail(pooled_heads, map_wo, map_bo, map_ln_gain, map_ln_bias, map_w_up, map_b_up, map_w_down, map_b_down)

    return jax.shard_map(local_program, mesh=mesh, in_specs=in_specs, out_specs=P('dp', None), check_vma=False)
```

```python
import functools

import jax
import jax.numpy as jnp
from jax import lax
from jax.experimental import pallas as pl
from jax.experimental.layout import Layout, with_layout_constraint
from jax.experimental.pallas import tpu as pltpu
from jax.sharding import PartitionSpec as P

LN_EPS = 1e-6
LOG2E = 1.4426950408889634
LANES = 128
BF16_MAX = 3.3895313892515355e38


def layer_norm(values, gain_vec, bias_vec):
    centered = values - jnp.mean(values, axis=-1, keepdims=True)
    variance = jnp.mean(centered * centered, axis=-1, keepdims=True)
    return centered * lax.rsqrt(variance + LN_EPS) * gain_vec + bias_vec


def row_major(values):
    return with_layout_constraint(values, Layout(major_to_minor=tuple(range(values.ndim))))


def round_up(size, multiple):
    return -(-size // multiple) * multiple


def attention_kernel(head_dim, chunk, q_ref, k_own_ref, k_far_ref, v_own_ref, v_far_ref, v_own_last_ref, v_far_last_ref, *refs):
    out_ref, scores_a, scores_b, max_a, max_b, first_out, apart = refs[-7:]
    half_keys = k_own_ref.shape[1]
    block = q_ref.shape[1] // 2
    step = pl.program_id(0)
    exp_scale = head_dim ** -0.5 * LOG2E

    def score_chunk(keys_t, queries, rows, scores, running):
        part = lax.dot_general(keys_t, queries, (((0,), (0,)), ((), ())), preferred_element_type=jnp.float32)
        scores[rows, :] = part
        part_max = jnp.max(part.reshape(chunk // 8, 8, block), axis=0)
        return part_max if running is None else jnp.maximum(running, part_max)

    def mix_chunk(values, rows, scores, peak, total, mixed):
        weights = jnp.exp2((scores[rows, :] - peak) * exp_scale)
        part_total = jnp.sum(weights.reshape(chunk // 8, 8, block), axis=0)
        part_mixed = jnp.dot(values, weights.astype(jnp.bfloat16), preferred_element_type=jnp.float32)
        if total is None:
            return part_total, part_mixed
        return total + part_total, mixed + part_mixed

    def overlap(query_slot, score_buf, max_buf, v_own, v_far, mix_buf, mix_max):
        running, total, mixed = None, None, None
        peak = jnp.max(mix_max[...], axis=0, keepdims=True)
        queries = q_ref[:, query_slot * block:(query_slot + 1) * block]
        for half, (k_ref, v_ref) in enumerate(((k_own_ref, v_own), (k_far_ref, v_far))):
            for start in range(0, half_keys, chunk):
                rows = pl.ds(half * half_keys + start, chunk)
                running = score_chunk(k_ref[:, start:start + chunk], queries, rows, score_buf, running)
                total, mixed = mix_chunk(v_ref[:, start:start + chunk], rows, mix_buf, peak, total, mixed)
        max_buf[...] = running
        return mixed[:head_dim] / jnp.sum(total, axis=0, keepdims=True)

    def write(rows, values_t):
        filled = jnp.concatenate([values_t, jnp.zeros((LANES - head_dim, block), jnp.float32)], axis=0)
        out_ref[rows, :] = filled.T.astype(out_ref.dtype)

    @pl.when(step == 0)
    def _():
        apart[0] = 0
        scores_b[...] = jnp.zeros_like(scores_b)
        max_b[...] = jnp.zeros_like(max_b)
        first_out[...] = jnp.zeros_like(first_out)

    @pl.when(apart[0] == 0)
    def _():
        second = overlap(0, scores_a, max_a, v_own_last_ref, v_far_last_ref, scores_b, max_b)
        write(slice(0, block), first_out[...])
        write(slice(block, 2 * block), second)

    @pl.when(apart[0] == 0)
    def _():
        first_out[...] = overlap(1, scores_b, max_b, v_own_ref, v_far_ref, scores_a, max_a)


def heads_attention(qkv_own, qkv_far, head_dim, heads, place, stride, previous, n_out):
    first, count = heads
    n_own = qkv_own.shape[1]
    pair = n_own // 2
    per_head = n_own // pair
    last = count * per_head - 1
    now = lambda i: first + jnp.minimum(i, last) // per_head
    before = lambda i: first + jnp.maximum(i - 1, 0) // per_head
    rows = round_up(head_dim, 16)
    whole = (rows, n_own)
    in_specs = [
        pl.BlockSpec((rows, pair), lambda i: (3 * now(i), jnp.minimum(i, last) % per_head)),
        pl.BlockSpec(whole, lambda i: (3 * now(i) + 1, 0)),
        pl.BlockSpec(whole, lambda i: (3 * now(i) + 1, 0)),
        pl.BlockSpec(whole, lambda i: (3 * now(i) + 2, 0)),
        pl.BlockSpec(whole, lambda i: (3 * now(i) + 2, 0)),
        pl.BlockSpec(whole, lambda i: (3 * before(i) + 2, 0)),
        pl.BlockSpec(whole, lambda i: (3 * before(i) + 2, 0)),
    ]
    operands = [qkv_own, qkv_own, qkv_far, qkv_own, qkv_far, qkv_own, qkv_far]
    aliases = {}
    if previous is not None:
        in_specs.append(pl.BlockSpec(memory_space=pl.ANY))
        operands.append(previous)
        aliases = {7: 0}
    scored = count * n_own * 2 * n_own
    return pl.pallas_call(
        functools.partial(attention_kernel, head_dim, 256),
        grid=(last + 2,),
        out_shape=jax.ShapeDtypeStruct((n_own, n_out * LANES), jnp.bfloat16),
        in_specs=in_specs,
        out_specs=pl.BlockSpec((pair, LANES), lambda i: (jnp.maximum(i - 1, 0) % per_head, place + stride * before(i))),
        scratch_shapes=[
            pltpu.VMEM((2 * n_own, pair // 2), jnp.float32),
            pltpu.VMEM((2 * n_own, pair // 2), jnp.float32),
            pltpu.VMEM((8, pair // 2), jnp.float32),
            pltpu.VMEM((8, pair // 2), jnp.float32),
            pltpu.VMEM((head_dim, pair // 2), jnp.float32),
            pltpu.SMEM((1,), jnp.int32),
        ],
        input_output_aliases=aliases,
        compiler_params=pltpu.CompilerParams(dimension_semantics=('arbitrary',), vmem_limit_bytes=40 * 1024 * 1024),
        cost_estimate=pl.CostEstimate(flops=4 * scored * LANES, bytes_accessed=8 * 1024 * 1024, transcendentals=scored),
        name='heads_attention',
    )(*operands)


def project_kernel(x_ref, gain_ref, shift_ref, weight_ref, bias_ref, out_ref):
    hidden = layer_norm(x_ref[...].astype(jnp.float32), gain_ref[...], shift_ref[...]).astype(jnp.bfloat16)
    product = lax.dot_general(weight_ref[...], hidden, (((1,), (1,)), ((), ())), preferred_element_type=jnp.float32)
    out_ref[...] = (product + bias_ref[...]).astype(out_ref.dtype)


def project_tokens(resid, gain, shift, weight, bias, block=256):
    n_own, width = resid.shape
    rows = weight.shape[0]
    fixed = lambda shape: pl.BlockSpec(shape, lambda i: (0, 0))
    return pl.pallas_call(
        project_kernel,
        grid=(n_own // block,),
        out_shape=jax.ShapeDtypeStruct((rows, n_own), jnp.bfloat16),
        in_specs=[pl.BlockSpec((block, width), lambda i: (i, 0)), fixed((1, width)), fixed((1, width)), fixed((rows, width)), fixed((rows, 1))],
        out_specs=pl.BlockSpec((rows, block), lambda i: (0, i)),
        compiler_params=pltpu.CompilerParams(dimension_semantics=('arbitrary',), vmem_limit_bytes=32 * 1024 * 1024),
        cost_estimate=pl.CostEstimate(flops=2 * n_own * width * rows, bytes_accessed=2 * (n_own * width + rows * width + rows * n_own), transcendentals=n_own),
        name='project_tokens',
    )(resid, gain[None], shift[None], weight, bias)


def split_three(values):
    high = lax.reduce_precision(jnp.clip(values, -BF16_MAX, BF16_MAX), 8, 7)
    middle = lax.reduce_precision(values - high, 8, 7)
    return [high.astype(jnp.bfloat16), middle.astype(jnp.bfloat16), (values - high - middle).astype(jnp.bfloat16)]


def join_three(parts):
    high, middle, low = (part.astype(jnp.float32) for part in parts)
    return high + middle + low


def map_tail(pooled_heads, map_wo, map_bo, map_ln_gain, map_ln_bias, map_w_up, map_b_up, map_w_down, map_b_down):
    attn_vec = jnp.einsum('bhe,hed->bd', pooled_heads, map_wo, preferred_element_type=jnp.float32) + map_bo
    map_hidden = layer_norm(attn_vec, map_ln_gain, map_ln_bias).astype(jnp.bfloat16)
    map_act = jax.nn.gelu(jnp.dot(map_hidden, map_w_up, preferred_element_type=jnp.float32) + map_b_up, approximate=True).astype(jnp.bfloat16)
    return (attn_vec + jnp.dot(map_act, map_w_down, preferred_element_type=jnp.float32) + map_b_down).astype(jnp.bfloat16)


def solution(mesh):
    tp_size = mesh.shape['tp']
    in_specs = (P('dp', 'tp', None), P(), P(), P(None, None, 'tp', None), P(None, 'tp', None), P('tp', None, None), P(), P(), P(), P(None, 'tp'), P('tp'), P('tp', None)) + (P(),) * 16
    partner = [(device, device ^ 1) for device in range(tp_size)]

    def local_program(tokens, ln1_gain, ln1_bias, w_qkv, b_qkv, w_out, b_out, ln2_gain, ln2_bias, w_up, b_up, w_down, b_down, lnf_gain, lnf_bias, probe_vec, map_wq, map_bq, map_wkv, map_bkv, map_wo, map_bo, map_ln_gain, map_ln_bias, map_w_up, map_b_up, map_w_down, map_b_down):
        n_images, run, width = tokens.shape
        groups, head_dim = w_qkv.shape[2:]
        n_heads = groups * tp_size
        hidden_units = w_up.shape[1]
        own = n_images * run

        resid = row_major(lax.all_to_all(row_major(tokens.reshape(tp_size, own // tp_size, width)), 'tp', split_axis=0, concat_axis=0, tiled=True).reshape(own, width))

        rows_padded = round_up(head_dim, 16)
        shards = []
        for group in range(groups):
            rows = jnp.transpose(w_qkv[:, :, group], (1, 2, 0))
            bias_row = jnp.concatenate(split_three(b_qkv[:, group].reshape(3 * head_dim)))
            bias_row = jnp.pad(bias_row, (0, width - bias_row.shape[0]))[None]
            extra = jnp.pad(bias_row, ((0, rows_padded - head_dim - 1), (0, 0)))
            none = jnp.zeros_like(extra)
            shards.append(jnp.concatenate([rows[0], none, rows[1], none, rows[2], extra], axis=0))
        padded = round_up(hidden_units, 32)
        w_up_t = jnp.pad(w_up.T, ((0, padded - hidden_units), (0, 0)))
        high, middle, low = split_three(b_up)
        up_rows = jnp.stack([jnp.pad(jnp.concatenate([high, middle]), (0, width - 2 * hidden_units)), jnp.pad(low, (0, width - hidden_units))])
        w_down_p = jnp.pad(jnp.concatenate([w_down, up_rows], axis=0), ((0, padded - hidden_units - 2), (0, 0)))

        gathered = [lax.all_gather(shards[0], 'tp', axis=0, tiled=True)]
        resid, later, w_out, w_up_t, w_down_p = lax.optimization_barrier((resid, shards[1:], w_out, w_up_t, w_down_p))
        gathered += [lax.all_gather(shard, 'tp', axis=0, tiled=True) for shard in later]
        w_out_all = lax.all_gather(w_out.reshape(groups * head_dim, width), 'tp', axis=0, tiled=True)
        w_up_all = lax.all_gather(w_up_t, 'tp', axis=0, tiled=True)
        w_down_all = lax.all_gather(w_down_p, 'tp', axis=0, tiled=True)

        def projections(group, resid):
            bias_row = gathered[group].reshape(tp_size, 3 * rows_padded, width)[:, 2 * rows_padded + head_dim, :9 * head_dim]
            bias_row = bias_row.reshape(tp_size, 3, 3, head_dim)
            bias = join_three([bias_row[:, part] for part in range(3)])
            bias = jnp.pad(bias, ((0, 0), (0, 0), (0, rows_padded - head_dim))).reshape(-1, 1)
            qkv_t = project_tokens(resid, ln1_gain, ln1_bias, gathered[group], bias)
            return qkv_t, lax.ppermute(qkv_t, 'tp', partner)

        half = tp_size // 2
        first_group = projections(0, resid)
        mixed = heads_attention(*first_group, head_dim, (0, half), 0, groups, None, n_heads)
        mixed, resid_later = lax.optimization_barrier((mixed, resid))
        second_group = projections(1, resid_later)
        mixed = heads_attention(*first_group, head_dim, (half, half), 0, groups, mixed, n_heads)
        mixed = heads_attention(*second_group, head_dim, (0, tp_size), 1, groups, mixed, n_heads)

        w_out_rows = jnp.pad(w_out_all.reshape(n_heads, head_dim, width), ((0, 0), (0, LANES - head_dim), (0, 0))).reshape(n_heads * LANES, width)
        attn_local = jnp.dot(mixed, w_out_rows, preferred_element_type=jnp.float32)
        resid_one = row_major((resid.astype(jnp.float32) + attn_local + b_out).astype(jnp.bfloat16))
        hidden_two = layer_norm(resid_one.astype(jnp.float32), ln2_gain, ln2_bias).astype(jnp.bfloat16)
        bias_rows = w_down_all.reshape(tp_size, padded, width)[:, hidden_units:hidden_units + 2]
        b_up_all = join_three([bias_rows[:, 0, :hidden_units], bias_rows[:, 0, hidden_units:2 * hidden_units], bias_rows[:, 1, :hidden_units]])
        b_up_all = jnp.pad(b_up_all, ((0, 0), (0, padded - hidden_units))).reshape(tp_size * padded)
        pre_act = lax.dot_general(hidden_two, w_up_all, (((1,), (1,)), ((), ())), preferred_element_type=jnp.float32) + b_up_all
        activated = jax.nn.gelu(pre_act, approximate=True).astype(jnp.bfloat16)
        mlp_local = jnp.dot(activated, w_down_all, preferred_element_type=jnp.float32)
        resid_two = row_major((resid_one.astype(jnp.float32) + mlp_local + b_down).astype(jnp.bfloat16))
        encoded = layer_norm(resid_two.astype(jnp.float32), lnf_gain, lnf_bias).astype(jnp.bfloat16)

        probe_q = (jnp.dot(probe_vec[None], map_wq.reshape(width, width), preferred_element_type=jnp.float32)[0] + map_bq.reshape(width)).astype(jnp.bfloat16)
        head_of = jnp.arange(width) // head_dim
        on_head = head_of[:, None] == jnp.arange(n_heads)[None]
        probe_cols = jnp.where(on_head, probe_q[:, None], jnp.zeros((), jnp.bfloat16))
        map_keys = (jnp.dot(encoded, map_wkv[:, 0].reshape(width, width), preferred_element_type=jnp.float32) + map_bkv[0].reshape(width)).astype(jnp.bfloat16)
        map_vals = (jnp.dot(encoded, map_wkv[:, 1].reshape(width, width), preferred_element_type=jnp.float32) + map_bkv[1].reshape(width)).astype(jnp.bfloat16)
        scores = lax.dot_general(probe_cols, map_keys, (((0,), (1,)), ((), ())), preferred_element_type=jnp.float32) * head_dim ** -0.5
        peak = jnp.max(scores, axis=-1, keepdims=True)
        weights = jnp.exp(scores - peak)
        total = jnp.sum(weights, axis=-1, keepdims=True)
        every_head = jnp.dot(weights.astype(jnp.bfloat16), map_vals, preferred_element_type=jnp.float32)
        pooled = jnp.sum(jnp.where(on_head.T, every_head, 0.0).reshape(n_heads, n_heads, head_dim), axis=1)
        parts = lax.all_gather(jnp.concatenate([pooled, total, peak], axis=-1), 'tp', axis=0, tiled=False)
        parts = parts.reshape(n_images, tp_size // n_images, n_heads, head_dim + 2)
        pooled_all, total_all, peak_all = parts[..., :head_dim], parts[..., head_dim:head_dim + 1], parts[..., head_dim + 1:]
        share = jnp.exp(peak_all - jnp.max(peak_all, axis=1, keepdims=True))
        pooled_heads = (jnp.sum(pooled_all * share, axis=1) / jnp.sum(total_all * share, axis=1)).astype(jnp.bfloat16)
        return map_tail(pooled_heads, map_wo, map_bo, map_ln_gain, map_ln_bias, map_w_up, map_b_up, map_w_down, map_b_down)

    return jax.shard_map(local_program, mesh=mesh, in_specs=in_specs, out_specs=P('dp', None), check_vma=False)
```

```python
import functools

import jax
import jax.numpy as jnp
from jax import lax
from jax.experimental import pallas as pl
from jax.experimental.layout import Layout, with_layout_constraint
from jax.experimental.pallas import tpu as pltpu
from jax.sharding import PartitionSpec as P

LN_EPS = 1e-6
LOG2E = 1.4426950408889634
LANES = 128
BF16_MAX = 3.3895313892515355e38


def layer_norm(values, gain_vec, bias_vec):
    centered = values - jnp.mean(values, axis=-1, keepdims=True)
    variance = jnp.mean(centered * centered, axis=-1, keepdims=True)
    return centered * lax.rsqrt(variance + LN_EPS) * gain_vec + bias_vec


def row_major(values):
    return with_layout_constraint(values, Layout(major_to_minor=tuple(range(values.ndim))))


def round_up(size, multiple):
    return -(-size // multiple) * multiple


def attention_kernel(head_dim, chunk, q_ref, k_own_ref, k_far_ref, v_own_ref, v_far_ref, v_own_last_ref, v_far_last_ref, *refs):
    out_ref, scores_a, scores_b, max_a, max_b, first_out, apart = refs[-7:]
    half_keys = k_own_ref.shape[1]
    block = q_ref.shape[1] // 2
    step = pl.program_id(0)
    exp_scale = head_dim ** -0.5 * LOG2E

    def score_chunk(keys_t, queries, rows, scores, running):
        part = lax.dot_general(keys_t, queries, (((0,), (0,)), ((), ())), preferred_element_type=jnp.float32)
        scores[rows, :] = part
        part_max = jnp.max(part.reshape(chunk // 8, 8, block), axis=0)
        return part_max if running is None else jnp.maximum(running, part_max)

    def mix_chunk(values, rows, scores, peak, total, mixed):
        weights = jnp.exp2((scores[rows, :] - peak) * exp_scale)
        part_total = jnp.sum(weights.reshape(chunk // 8, 8, block), axis=0)
        part_mixed = jnp.dot(values, weights.astype(jnp.bfloat16), preferred_element_type=jnp.float32)
        if total is None:
            return part_total, part_mixed
        return total + part_total, mixed + part_mixed

    def overlap(query_slot, score_buf, max_buf, v_own, v_far, mix_buf, mix_max):
        running, total, mixed = None, None, None
        peak = jnp.max(mix_max[...], axis=0, keepdims=True)
        queries = q_ref[:, query_slot * block:(query_slot + 1) * block]
        for half, (k_ref, v_ref) in enumerate(((k_own_ref, v_own), (k_far_ref, v_far))):
            for start in range(0, half_keys, chunk):
                rows = pl.ds(half * half_keys + start, chunk)
                running = score_chunk(k_ref[:, start:start + chunk], queries, rows, score_buf, running)
                total, mixed = mix_chunk(v_ref[:, start:start + chunk], rows, mix_buf, peak, total, mixed)
        max_buf[...] = running
        return mixed[:head_dim] / jnp.sum(total, axis=0, keepdims=True)

    def write(rows, values_t):
        filled = jnp.concatenate([values_t, jnp.zeros((LANES - head_dim, block), jnp.float32)], axis=0)
        out_ref[rows, :] = filled.T.astype(out_ref.dtype)

    @pl.when(step == 0)
    def _():
        apart[0] = 0
        scores_b[...] = jnp.zeros_like(scores_b)
        max_b[...] = jnp.zeros_like(max_b)
        first_out[...] = jnp.zeros_like(first_out)

    @pl.when(apart[0] == 0)
    def _():
        second = overlap(0, scores_a, max_a, v_own_last_ref, v_far_last_ref, scores_b, max_b)
        write(slice(0, block), first_out[...])
        write(slice(block, 2 * block), second)

    @pl.when(step < pl.num_programs(0) - 1)
    def _():
        first_out[...] = overlap(1, scores_b, max_b, v_own_ref, v_far_ref, scores_a, max_a)


def heads_attention(qkv_own, qkv_far, head_dim, heads, place, stride, previous, n_out):
    first, count = heads
    n_own = qkv_own.shape[1]
    pair = n_own // 2
    per_head = n_own // pair
    last = count * per_head - 1
    now = lambda i: first + jnp.minimum(i, last) // per_head
    before = lambda i: first + jnp.maximum(i - 1, 0) // per_head
    rows = round_up(head_dim, 16)
    whole = (rows, n_own)
    in_specs = [
        pl.BlockSpec((rows, pair), lambda i: (3 * now(i), jnp.minimum(i, last) % per_head)),
        pl.BlockSpec(whole, lambda i: (3 * now(i) + 1, 0)),
        pl.BlockSpec(whole, lambda i: (3 * now(i) + 1, 0)),
        pl.BlockSpec(whole, lambda i: (3 * now(i) + 2, 0)),
        pl.BlockSpec(whole, lambda i: (3 * now(i) + 2, 0)),
        pl.BlockSpec(whole, lambda i: (3 * before(i) + 2, 0)),
        pl.BlockSpec(whole, lambda i: (3 * before(i) + 2, 0)),
    ]
    operands = [qkv_own, qkv_own, qkv_far, qkv_own, qkv_far, qkv_own, qkv_far]
    aliases = {}
    if previous is not None:
        in_specs.append(pl.BlockSpec(memory_space=pl.ANY))
        operands.append(previous)
        aliases = {7: 0}
    scored = count * n_own * 2 * n_own
    return pl.pallas_call(
        functools.partial(attention_kernel, head_dim, 256),
        grid=(last + 2,),
        out_shape=jax.ShapeDtypeStruct((n_own, n_out * LANES), jnp.bfloat16),
        in_specs=in_specs,
        out_specs=pl.BlockSpec((pair, LANES), lambda i: (jnp.maximum(i - 1, 0) % per_head, place + stride * before(i))),
        scratch_shapes=[
            pltpu.VMEM((2 * n_own, pair // 2), jnp.float32),
            pltpu.VMEM((2 * n_own, pair // 2), jnp.float32),
            pltpu.VMEM((8, pair // 2), jnp.float32),
            pltpu.VMEM((8, pair // 2), jnp.float32),
            pltpu.VMEM((head_dim, pair // 2), jnp.float32),
            pltpu.SMEM((1,), jnp.int32),
        ],
        input_output_aliases=aliases,
        compiler_params=pltpu.CompilerParams(dimension_semantics=('arbitrary',), vmem_limit_bytes=40 * 1024 * 1024),
        cost_estimate=pl.CostEstimate(flops=4 * scored * LANES, bytes_accessed=8 * 1024 * 1024, transcendentals=scored),
        name='heads_attention',
    )(*operands)


def project_kernel(x_ref, gain_ref, shift_ref, weight_ref, bias_ref, out_ref):
    hidden = layer_norm(x_ref[...].astype(jnp.float32), gain_ref[...], shift_ref[...]).astype(jnp.bfloat16)
    product = lax.dot_general(weight_ref[...], hidden, (((1,), (1,)), ((), ())), preferred_element_type=jnp.float32)
    out_ref[...] = (product + bias_ref[...]).astype(out_ref.dtype)


def project_tokens(resid, gain, shift, weight, bias, block=512):
    n_own, width = resid.shape
    rows = weight.shape[0]
    fixed = lambda shape: pl.BlockSpec(shape, lambda i: (0, 0))
    return pl.pallas_call(
        project_kernel,
        grid=(n_own // block,),
        out_shape=jax.ShapeDtypeStruct((rows, n_own), jnp.bfloat16),
        in_specs=[pl.BlockSpec((block, width), lambda i: (i, 0)), fixed((1, width)), fixed((1, width)), fixed((rows, width)), fixed((rows, 1))],
        out_specs=pl.BlockSpec((rows, block), lambda i: (0, i)),
        compiler_params=pltpu.CompilerParams(dimension_semantics=('arbitrary',), vmem_limit_bytes=32 * 1024 * 1024),
        cost_estimate=pl.CostEstimate(flops=2 * n_own * width * rows, bytes_accessed=2 * (n_own * width + rows * width + rows * n_own), transcendentals=n_own),
        name='project_tokens',
    )(resid, gain[None], shift[None], weight, bias)


def split_three(values):
    high = lax.reduce_precision(jnp.clip(values, -BF16_MAX, BF16_MAX), 8, 7)
    middle = lax.reduce_precision(values - high, 8, 7)
    return [high.astype(jnp.bfloat16), middle.astype(jnp.bfloat16), (values - high - middle).astype(jnp.bfloat16)]


def join_three(parts):
    high, middle, low = (part.astype(jnp.float32) for part in parts)
    return high + middle + low


def map_tail(pooled_heads, map_wo, map_bo, map_ln_gain, map_ln_bias, map_w_up, map_b_up, map_w_down, map_b_down):
    attn_vec = jnp.einsum('bhe,hed->bd', pooled_heads, map_wo, preferred_element_type=jnp.float32) + map_bo
    map_hidden = layer_norm(attn_vec, map_ln_gain, map_ln_bias).astype(jnp.bfloat16)
    map_act = jax.nn.gelu(jnp.dot(map_hidden, map_w_up, preferred_element_type=jnp.float32) + map_b_up, approximate=True).astype(jnp.bfloat16)
    return (attn_vec + jnp.dot(map_act, map_w_down, preferred_element_type=jnp.float32) + map_b_down).astype(jnp.bfloat16)


def solution(mesh):
    tp_size = mesh.shape['tp']
    in_specs = (P('dp', 'tp', None), P(), P(), P(None, None, 'tp', None), P(None, 'tp', None), P('tp', None, None), P(), P(), P(), P(None, 'tp'), P('tp'), P('tp', None)) + (P(),) * 16
    partner = [(device, device ^ 1) for device in range(tp_size)]

    def local_program(tokens, ln1_gain, ln1_bias, w_qkv, b_qkv, w_out, b_out, ln2_gain, ln2_bias, w_up, b_up, w_down, b_down, lnf_gain, lnf_bias, probe_vec, map_wq, map_bq, map_wkv, map_bkv, map_wo, map_bo, map_ln_gain, map_ln_bias, map_w_up, map_b_up, map_w_down, map_b_down):
        n_images, run, width = tokens.shape
        groups, head_dim = w_qkv.shape[2:]
        n_heads = groups * tp_size
        hidden_units = w_up.shape[1]
        own = n_images * run

        resid = row_major(lax.all_to_all(row_major(tokens.reshape(tp_size, own // tp_size, width)), 'tp', split_axis=0, concat_axis=0, tiled=True).reshape(own, width))

        rows_padded = round_up(head_dim, 16)
        shards = []
        for group in range(groups):
            rows = jnp.transpose(w_qkv[:, :, group], (1, 2, 0))
            bias_row = jnp.concatenate(split_three(b_qkv[:, group].reshape(3 * head_dim)))
            bias_row = jnp.pad(bias_row, (0, width - bias_row.shape[0]))[None]
            extra = jnp.pad(bias_row, ((0, rows_padded - head_dim - 1), (0, 0)))
            none = jnp.zeros_like(extra)
            shards.append(jnp.concatenate([rows[0], none, rows[1], none, rows[2], extra], axis=0))
        padded = round_up(hidden_units, 32)
        w_up_t = jnp.pad(w_up.T, ((0, padded - hidden_units), (0, 0)))
        high, middle, low = split_three(b_up)
        up_rows = jnp.stack([jnp.pad(jnp.concatenate([high, middle]), (0, width - 2 * hidden_units)), jnp.pad(low, (0, width - hidden_units))])
        w_down_p = jnp.pad(jnp.concatenate([w_down, up_rows], axis=0), ((0, padded - hidden_units - 2), (0, 0)))

        gathered = [lax.all_gather(shards[0], 'tp', axis=0, tiled=True)]
        probe_q = (jnp.dot(probe_vec[None], map_wq.reshape(width, width), preferred_element_type=jnp.float32)[0] + map_bq.reshape(width)).astype(jnp.bfloat16)
        head_of = jnp.arange(width) // head_dim
        on_head = head_of[:, None] == jnp.arange(n_heads)[None]
        probe_cols = jnp.where(on_head, probe_q[:, None], jnp.zeros((), jnp.bfloat16))
        pool_wk, pool_wv = map_wkv[:, 0].reshape(width, width), map_wkv[:, 1].reshape(width, width)
        w_out_p = jnp.pad(w_out, ((0, 0), (0, LANES - head_dim), (0, 0))).reshape(groups * LANES, width)
        resid, later, w_out_p, w_up_t, w_down_p, probe_cols, pool_wk, pool_wv = lax.optimization_barrier(
            (resid, shards[1:], w_out_p, w_up_t, w_down_p, probe_cols, pool_wk, pool_wv))
        gathered += [lax.all_gather(shard, 'tp', axis=0, tiled=True) for shard in later]
        w_out_all = lax.all_gather(w_out_p, 'tp', axis=0, tiled=True)
        w_up_all = lax.all_gather(w_up_t, 'tp', axis=0, tiled=True)
        w_down_all = lax.all_gather(w_down_p, 'tp', axis=0, tiled=True)

        def projections(group, resid):
            bias_row = gathered[group].reshape(tp_size, 3 * rows_padded, width)[:, 2 * rows_padded + head_dim, :9 * head_dim]
            bias_row = bias_row.reshape(tp_size, 3, 3, head_dim)
            bias = join_three([bias_row[:, part] for part in range(3)])
            bias = jnp.pad(bias, ((0, 0), (0, 0), (0, rows_padded - head_dim))).reshape(-1, 1)
            qkv_t = project_tokens(resid, ln1_gain, ln1_bias, gathered[group], bias)
            return qkv_t, lax.ppermute(qkv_t, 'tp', partner)

        half = tp_size // 2
        first_group = projections(0, resid)
        mixed = heads_attention(*first_group, head_dim, (0, half), 0, groups, None, n_heads)
        mixed, resid_later, gathered[1] = lax.optimization_barrier((mixed, resid, gathered[1]))
        second_group = projections(1, resid_later)
        mixed = heads_attention(*first_group, head_dim, (half, half), 0, groups, mixed, n_heads)
        mixed = heads_attention(*second_group, head_dim, (0, tp_size), 1, groups, mixed, n_heads)

        attn_local = jnp.dot(mixed, w_out_all, preferred_element_type=jnp.float32)
        resid_one = row_major((resid.astype(jnp.float32) + attn_local + b_out).astype(jnp.bfloat16))
        hidden_two = layer_norm(resid_one.astype(jnp.float32), ln2_gain, ln2_bias).astype(jnp.bfloat16)
        bias_rows = w_down_all.reshape(tp_size, padded, width)[:, hidden_units:hidden_units + 2]
        b_up_all = join_three([bias_rows[:, 0, :hidden_units], bias_rows[:, 0, hidden_units:2 * hidden_units], bias_rows[:, 1, :hidden_units]])
        b_up_all = jnp.pad(b_up_all, ((0, 0), (0, padded - hidden_units))).reshape(tp_size * padded)
        pre_act = lax.dot_general(hidden_two, w_up_all, (((1,), (1,)), ((), ())), preferred_element_type=jnp.float32) + b_up_all
        activated = jax.nn.gelu(pre_act, approximate=True).astype(jnp.bfloat16)
        mlp_local = jnp.dot(activated, w_down_all, preferred_element_type=jnp.float32)
        resid_two = row_major((resid_one.astype(jnp.float32) + mlp_local + b_down).astype(jnp.bfloat16))
        encoded = layer_norm(resid_two.astype(jnp.float32), lnf_gain, lnf_bias).astype(jnp.bfloat16)

        map_keys = (jnp.dot(encoded, pool_wk, preferred_element_type=jnp.float32) + map_bkv[0].reshape(width)).astype(jnp.bfloat16)
        map_vals = (jnp.dot(encoded, pool_wv, preferred_element_type=jnp.float32) + map_bkv[1].reshape(width)).astype(jnp.bfloat16)
        scores = lax.dot_general(probe_cols, map_keys, (((0,), (1,)), ((), ())), preferred_element_type=jnp.float32) * head_dim ** -0.5
        peak = jnp.max(scores, axis=-1, keepdims=True)
        weights = jnp.exp(scores - peak)
        total = jnp.sum(weights, axis=-1, keepdims=True)
        every_head = jnp.dot(weights.astype(jnp.bfloat16), map_vals, preferred_element_type=jnp.float32)
        pooled = jnp.sum(jnp.where(on_head.T, every_head, 0.0).reshape(n_heads, n_heads, head_dim), axis=1)
        parts = lax.all_gather(jnp.concatenate([pooled, total, peak], axis=-1), 'tp', axis=0, tiled=False)
        parts = parts.reshape(n_images, tp_size // n_images, n_heads, head_dim + 2)
        pooled_all, total_all, peak_all = parts[..., :head_dim], parts[..., head_dim:head_dim + 1], parts[..., head_dim + 1:]
        share = jnp.exp(peak_all - jnp.max(peak_all, axis=1, keepdims=True))
        pooled_heads = (jnp.sum(pooled_all * share, axis=1) / jnp.sum(total_all * share, axis=1)).astype(jnp.bfloat16)
        return map_tail(pooled_heads, map_wo, map_bo, map_ln_gain, map_ln_bias, map_w_up, map_b_up, map_w_down, map_b_down)

    return jax.shard_map(local_program, mesh=mesh, in_specs=in_specs, out_specs=P('dp', None), check_vma=False)
```

```python
import functools

import jax
import jax.numpy as jnp
from jax import lax
from jax.experimental import pallas as pl
from jax.experimental.layout import Layout, with_layout_constraint
from jax.experimental.pallas import tpu as pltpu
from jax.sharding import PartitionSpec as P

LN_EPS = 1e-6
LOG2E = 1.4426950408889634
LANES = 128
BF16_MAX = 3.3895313892515355e38


def layer_norm(values, gain_vec, bias_vec):
    centered = values - jnp.mean(values, axis=-1, keepdims=True)
    variance = jnp.mean(centered * centered, axis=-1, keepdims=True)
    return centered * lax.rsqrt(variance + LN_EPS) * gain_vec + bias_vec


def row_major(values):
    return with_layout_constraint(values, Layout(major_to_minor=tuple(range(values.ndim))))


def round_up(size, multiple):
    return -(-size // multiple) * multiple


def attention_kernel(head_dim, chunk, q_ref, k_own_ref, k_far_ref, v_own_ref, v_far_ref, v_own_last_ref, v_far_last_ref, *refs):
    out_ref, scores_a, scores_b, max_a, max_b, first_out, apart = refs[-7:]
    half_keys = k_own_ref.shape[1]
    block = q_ref.shape[1] // 2
    step = pl.program_id(0)
    exp_scale = head_dim ** -0.5 * LOG2E

    def score_chunk(keys_t, queries, rows, scores, running):
        part = lax.dot_general(keys_t, queries, (((0,), (0,)), ((), ())), preferred_element_type=jnp.float32)
        scores[rows, :] = part
        part_max = jnp.max(part.reshape(chunk // 8, 8, block), axis=0)
        return part_max if running is None else jnp.maximum(running, part_max)

    def mix_chunk(values, rows, scores, peak, total, mixed):
        weights = jnp.exp2((scores[rows, :] - peak) * exp_scale)
        part_total = jnp.sum(weights.reshape(chunk // 8, 8, block), axis=0)
        part_mixed = jnp.dot(values, weights.astype(jnp.bfloat16), preferred_element_type=jnp.float32)
        if total is None:
            return part_total, part_mixed
        return total + part_total, mixed + part_mixed

    def overlap(query_slot, score_buf, max_buf, v_own, v_far, mix_buf, mix_max):
        running, total, mixed = None, None, None
        peak = jnp.max(mix_max[...], axis=0, keepdims=True)
        queries = q_ref[:, query_slot * block:(query_slot + 1) * block]
        for half, (k_ref, v_ref) in enumerate(((k_own_ref, v_own), (k_far_ref, v_far))):
            for start in range(0, half_keys, chunk):
                rows = pl.ds(half * half_keys + start, chunk)
                running = score_chunk(k_ref[:, start:start + chunk], queries, rows, score_buf, running)
                total, mixed = mix_chunk(v_ref[:, start:start + chunk], rows, mix_buf, peak, total, mixed)
        max_buf[...] = running
        return mixed[:head_dim] / jnp.sum(total, axis=0, keepdims=True)

    def write(rows, values_t):
        filled = jnp.concatenate([values_t, jnp.zeros((LANES - head_dim, block), jnp.float32)], axis=0)
        out_ref[rows, :] = filled.T.astype(out_ref.dtype)

    @pl.when(step == 0)
    def _():
        apart[0] = 0
        scores_b[...] = jnp.zeros_like(scores_b)
        max_b[...] = jnp.zeros_like(max_b)
        first_out[...] = jnp.zeros_like(first_out)

    @pl.when(apart[0] == 0)
    def _():
        second = overlap(0, scores_a, max_a, v_own_last_ref, v_far_last_ref, scores_b, max_b)
        write(slice(0, block), first_out[...])
        write(slice(block, 2 * block), second)

    @pl.when(step < pl.num_programs(0) - 1)
    def _():
        first_out[...] = overlap(1, scores_b, max_b, v_own_ref, v_far_ref, scores_a, max_a)


def heads_attention(qkv_own, qkv_far, head_dim, heads, place, stride, previous, n_out):
    first, count = heads
    n_own = qkv_own.shape[1]
    pair = n_own // 2
    per_head = n_own // pair
    last = count * per_head - 1
    now = lambda i: first + jnp.minimum(i, last) // per_head
    before = lambda i: first + jnp.maximum(i - 1, 0) // per_head
    rows = round_up(head_dim, 16)
    whole = (rows, n_own)
    in_specs = [
        pl.BlockSpec((rows, pair), lambda i: (3 * now(i), jnp.minimum(i, last) % per_head)),
        pl.BlockSpec(whole, lambda i: (3 * now(i) + 1, 0)),
        pl.BlockSpec(whole, lambda i: (3 * now(i) + 1, 0)),
        pl.BlockSpec(whole, lambda i: (3 * now(i) + 2, 0)),
        pl.BlockSpec(whole, lambda i: (3 * now(i) + 2, 0)),
        pl.BlockSpec(whole, lambda i: (3 * before(i) + 2, 0)),
        pl.BlockSpec(whole, lambda i: (3 * before(i) + 2, 0)),
    ]
    operands = [qkv_own, qkv_own, qkv_far, qkv_own, qkv_far, qkv_own, qkv_far]
    aliases = {}
    if previous is not None:
        in_specs.append(pl.BlockSpec(memory_space=pl.ANY))
        operands.append(previous)
        aliases = {7: 0}
    scored = count * n_own * 2 * n_own
    return pl.pallas_call(
        functools.partial(attention_kernel, head_dim, 256),
        grid=(last + 2,),
        out_shape=jax.ShapeDtypeStruct((n_own, n_out * LANES), jnp.bfloat16),
        in_specs=in_specs,
        out_specs=pl.BlockSpec((pair, LANES), lambda i: (jnp.maximum(i - 1, 0) % per_head, place + stride * before(i))),
        scratch_shapes=[
            pltpu.VMEM((2 * n_own, pair // 2), jnp.float32),
            pltpu.VMEM((2 * n_own, pair // 2), jnp.float32),
            pltpu.VMEM((8, pair // 2), jnp.float32),
            pltpu.VMEM((8, pair // 2), jnp.float32),
            pltpu.VMEM((head_dim, pair // 2), jnp.float32),
            pltpu.SMEM((1,), jnp.int32),
        ],
        input_output_aliases=aliases,
        compiler_params=pltpu.CompilerParams(dimension_semantics=('arbitrary',), vmem_limit_bytes=40 * 1024 * 1024),
        cost_estimate=pl.CostEstimate(flops=4 * scored * LANES, bytes_accessed=8 * 1024 * 1024, transcendentals=scored),
        name='heads_attention',
    )(*operands)


def project_kernel(x_ref, gain_ref, shift_ref, weight_ref, bias_ref, out_ref):
    hidden = layer_norm(x_ref[...].astype(jnp.float32), gain_ref[...], shift_ref[...]).astype(jnp.bfloat16)
    product = lax.dot_general(weight_ref[...], hidden, (((1,), (1,)), ((), ())), preferred_element_type=jnp.float32)
    out_ref[...] = (product + bias_ref[...]).astype(out_ref.dtype)


def project_tokens(resid, gain, shift, weight, bias, block=512):
    n_own, width = resid.shape
    rows = weight.shape[0]
    fixed = lambda shape: pl.BlockSpec(shape, lambda i: (0, 0))
    return pl.pallas_call(
        project_kernel,
        grid=(n_own // block,),
        out_shape=jax.ShapeDtypeStruct((rows, n_own), jnp.bfloat16),
        in_specs=[pl.BlockSpec((block, width), lambda i: (i, 0)), fixed((1, width)), fixed((1, width)), fixed((rows, width)), fixed((rows, 1))],
        out_specs=pl.BlockSpec((rows, block), lambda i: (0, i)),
        compiler_params=pltpu.CompilerParams(dimension_semantics=('arbitrary',), vmem_limit_bytes=32 * 1024 * 1024),
        cost_estimate=pl.CostEstimate(flops=2 * n_own * width * rows, bytes_accessed=2 * (n_own * width + rows * width + rows * n_own), transcendentals=n_own),
        name='project_tokens',
    )(resid, gain[None], shift[None], weight, bias)


def split_three(values):
    high = lax.reduce_precision(jnp.clip(values, -BF16_MAX, BF16_MAX), 8, 7)
    middle = lax.reduce_precision(values - high, 8, 7)
    return [high.astype(jnp.bfloat16), middle.astype(jnp.bfloat16), (values - high - middle).astype(jnp.bfloat16)]


def join_three(parts):
    high, middle, low = (part.astype(jnp.float32) for part in parts)
    return high + middle + low


def finish_kernel(head_dim, up_chunk, mixed_ref, resid_ref, vec_ref, up_bias_ref, pool_bias_ref, probe_ref, w_out_hbm, w_up_hbm, w_down_hbm, wk_hbm, wv_hbm,
                  pooled_ref, total_ref, peak_ref, w_out, w_up, w_down, wk, wv, units, sems):
    step = pl.program_id(0)
    copies = [pltpu.make_async_copy(src, dst, sems.at[index]) for index, (src, dst) in enumerate(
        ((w_out_hbm, w_out), (w_up_hbm, w_up), (w_down_hbm, w_down), (wk_hbm, wk), (wv_hbm, wv)))]

    @pl.when(step == 0)
    def _():
        for copy in copies:
            copy.start()
        pooled_ref[...] = jnp.zeros_like(pooled_ref)
        total_ref[...] = jnp.zeros_like(total_ref)
        peak_ref[...] = jnp.full_like(peak_ref, -jnp.inf)

    def arrive(index):
        @pl.when(step == 0)
        def _():
            copies[index].wait()

    b_out, ln2_gain, ln2_bias, b_down, lnf_gain, lnf_bias = (vec_ref[index:index + 1, :] for index in range(6))
    arrive(0)
    attn_local = jnp.dot(mixed_ref[...], w_out[...], preferred_element_type=jnp.float32)
    resid_one = (resid_ref[...].astype(jnp.float32) + attn_local + b_out).astype(jnp.bfloat16)
    hidden_two = layer_norm(resid_one.astype(jnp.float32), ln2_gain, ln2_bias).astype(jnp.bfloat16)
    arrive(1)
    n_units = w_up.shape[0]
    for start in range(0, n_units, up_chunk):
        cols = slice(start, min(start + up_chunk, n_units))
        pre_act = lax.dot_general(hidden_two, w_up[cols, :], (((1,), (1,)), ((), ())), preferred_element_type=jnp.float32) + up_bias_ref[:, cols]
        units[:, cols] = jax.nn.gelu(pre_act, approximate=True).astype(jnp.bfloat16)
    arrive(2)
    mlp_local = jnp.dot(units[...], w_down[...], preferred_element_type=jnp.float32)
    resid_two = (resid_one.astype(jnp.float32) + mlp_local + b_down).astype(jnp.bfloat16)
    encoded = layer_norm(resid_two.astype(jnp.float32), lnf_gain, lnf_bias).astype(jnp.bfloat16)
    arrive(3)
    keys = (jnp.dot(encoded, wk[...], preferred_element_type=jnp.float32) + pool_bias_ref[0:1, :]).astype(jnp.bfloat16)
    arrive(4)
    values = (jnp.dot(encoded, wv[...], preferred_element_type=jnp.float32) + pool_bias_ref[1:2, :]).astype(jnp.bfloat16)
    scores = lax.dot_general(probe_ref[...], keys, (((1,), (1,)), ((), ())), preferred_element_type=jnp.float32) * head_dim ** -0.5
    peak = jnp.maximum(peak_ref[...], jnp.max(scores, axis=-1, keepdims=True))
    weights = jnp.exp(scores - peak)
    keep = jnp.exp(peak_ref[...] - peak)
    total_ref[...] = total_ref[...] * keep + jnp.sum(weights, axis=-1, keepdims=True)
    pooled_ref[...] = pooled_ref[...] * keep + jnp.dot(weights.astype(jnp.bfloat16), values, preferred_element_type=jnp.float32)
    peak_ref[...] = peak


def finish_tokens(mixed, resid, vectors, up_bias, pool_bias, probe, weights, head_dim, block=512):
    n_own, width = resid.shape
    n_heads = probe.shape[0]
    n_units = up_bias.shape[1]
    fixed = lambda shape: pl.BlockSpec(shape, lambda i: (0, 0))
    small = [vectors, up_bias, pool_bias, probe]
    return pl.pallas_call(
        functools.partial(finish_kernel, head_dim, 512),
        grid=(n_own // block,),
        out_shape=[jax.ShapeDtypeStruct((n_heads, columns), jnp.float32) for columns in (width, 1, 1)],
        in_specs=[pl.BlockSpec((block, mixed.shape[1]), lambda i: (i, 0)), pl.BlockSpec((block, width), lambda i: (i, 0))]
        + [fixed(array.shape) for array in small] + [pl.BlockSpec(memory_space=pl.ANY)] * len(weights),
        out_specs=[fixed((n_heads, columns)) for columns in (width, 1, 1)],
        scratch_shapes=[pltpu.VMEM(weight.shape, jnp.bfloat16) for weight in weights]
        + [pltpu.VMEM((block, n_units), jnp.bfloat16), pltpu.SemaphoreType.DMA((len(weights),))],
        compiler_params=pltpu.CompilerParams(dimension_semantics=('arbitrary',), vmem_limit_bytes=60 * 1024 * 1024),
        cost_estimate=pl.CostEstimate(flops=2 * n_own * sum(weight.size for weight in weights), bytes_accessed=40 * 1024 * 1024, transcendentals=n_own * n_units),
        name='finish_tokens',
    )(mixed, resid, *small, *weights)


def map_tail(pooled_heads, map_wo, map_bo, map_ln_gain, map_ln_bias, map_w_up, map_b_up, map_w_down, map_b_down):
    attn_vec = jnp.einsum('bhe,hed->bd', pooled_heads, map_wo, preferred_element_type=jnp.float32) + map_bo
    map_hidden = layer_norm(attn_vec, map_ln_gain, map_ln_bias).astype(jnp.bfloat16)
    map_act = jax.nn.gelu(jnp.dot(map_hidden, map_w_up, preferred_element_type=jnp.float32) + map_b_up, approximate=True).astype(jnp.bfloat16)
    return (attn_vec + jnp.dot(map_act, map_w_down, preferred_element_type=jnp.float32) + map_b_down).astype(jnp.bfloat16)


def solution(mesh):
    tp_size = mesh.shape['tp']
    in_specs = (P('dp', 'tp', None), P(), P(), P(None, None, 'tp', None), P(None, 'tp', None), P('tp', None, None), P(), P(), P(), P(None, 'tp'), P('tp'), P('tp', None)) + (P(),) * 16
    partner = [(device, device ^ 1) for device in range(tp_size)]

    def local_program(tokens, ln1_gain, ln1_bias, w_qkv, b_qkv, w_out, b_out, ln2_gain, ln2_bias, w_up, b_up, w_down, b_down, lnf_gain, lnf_bias, probe_vec, map_wq, map_bq, map_wkv, map_bkv, map_wo, map_bo, map_ln_gain, map_ln_bias, map_w_up, map_b_up, map_w_down, map_b_down):
        n_images, run, width = tokens.shape
        groups, head_dim = w_qkv.shape[2:]
        n_heads = groups * tp_size
        hidden_units = w_up.shape[1]
        own = n_images * run

        resid = row_major(lax.all_to_all(row_major(tokens.reshape(tp_size, own // tp_size, width)), 'tp', split_axis=0, concat_axis=0, tiled=True).reshape(own, width))

        rows_padded = round_up(head_dim, 16)
        shards = []
        for group in range(groups):
            rows = jnp.transpose(w_qkv[:, :, group], (1, 2, 0))
            bias_row = jnp.concatenate(split_three(b_qkv[:, group].reshape(3 * head_dim)))
            bias_row = jnp.pad(bias_row, (0, width - bias_row.shape[0]))[None]
            extra = jnp.pad(bias_row, ((0, rows_padded - head_dim - 1), (0, 0)))
            none = jnp.zeros_like(extra)
            shards.append(jnp.concatenate([rows[0], none, rows[1], none, rows[2], extra], axis=0))
        padded = round_up(hidden_units, 32)
        w_up_t = jnp.pad(w_up.T, ((0, padded - hidden_units), (0, 0)))
        high, middle, low = split_three(b_up)
        up_rows = jnp.stack([jnp.pad(jnp.concatenate([high, middle]), (0, width - 2 * hidden_units)), jnp.pad(low, (0, width - hidden_units))])
        w_down_p = jnp.pad(jnp.concatenate([w_down, up_rows], axis=0), ((0, padded - hidden_units - 2), (0, 0)))

        gathered = [lax.all_gather(shards[0], 'tp', axis=0, tiled=True)]
        probe_q = (jnp.dot(probe_vec[None], map_wq.reshape(width, width), preferred_element_type=jnp.float32)[0] + map_bq.reshape(width)).astype(jnp.bfloat16)
        head_of = jnp.arange(width) // head_dim
        on_head = head_of[:, None] == jnp.arange(n_heads)[None]
        probe_cols = jnp.where(on_head.T, probe_q[None], jnp.zeros((), jnp.bfloat16))
        pool_wk, pool_wv = map_wkv[:, 0].reshape(width, width), map_wkv[:, 1].reshape(width, width)
        w_out_p = jnp.pad(w_out, ((0, 0), (0, LANES - head_dim), (0, 0))).reshape(groups * LANES, width)
        resid, later, w_out_p, w_up_t, w_down_p, probe_cols, pool_wk, pool_wv = lax.optimization_barrier(
            (resid, shards[1:], w_out_p, w_up_t, w_down_p, probe_cols, pool_wk, pool_wv))
        gathered += [lax.all_gather(shard, 'tp', axis=0, tiled=True) for shard in later]
        w_out_all = lax.all_gather(w_out_p, 'tp', axis=0, tiled=True)
        w_up_all = lax.all_gather(w_up_t, 'tp', axis=0, tiled=True)
        w_down_all = lax.all_gather(w_down_p, 'tp', axis=0, tiled=True)

        def projections(group, resid):
            bias_row = gathered[group].reshape(tp_size, 3 * rows_padded, width)[:, 2 * rows_padded + head_dim, :9 * head_dim]
            bias_row = bias_row.reshape(tp_size, 3, 3, head_dim)
            bias = join_three([bias_row[:, part] for part in range(3)])
            bias = jnp.pad(bias, ((0, 0), (0, 0), (0, rows_padded - head_dim))).reshape(-1, 1)
            qkv_t = project_tokens(resid, ln1_gain, ln1_bias, gathered[group], bias)
            return qkv_t, lax.ppermute(qkv_t, 'tp', partner)

        half = tp_size // 2
        first_group = projections(0, resid)
        mixed = heads_attention(*first_group, head_dim, (0, half), 0, groups, None, n_heads)
        mixed, resid_later, gathered[1] = lax.optimization_barrier((mixed, resid, gathered[1]))
        second_group = projections(1, resid_later)
        mixed = heads_attention(*first_group, head_dim, (half, half), 0, groups, mixed, n_heads)
        mixed = heads_attention(*second_group, head_dim, (0, tp_size), 1, groups, mixed, n_heads)

        bias_rows = w_down_all.reshape(tp_size, padded, width)[:, hidden_units:hidden_units + 2]
        b_up_all = join_three([bias_rows[:, 0, :hidden_units], bias_rows[:, 0, hidden_units:2 * hidden_units], bias_rows[:, 1, :hidden_units]])
        b_up_all = jnp.pad(b_up_all, ((0, 0), (0, padded - hidden_units))).reshape(tp_size * padded)
        vectors = jnp.stack([b_out, ln2_gain, ln2_bias, b_down, lnf_gain, lnf_bias])
        every_head, total, peak = finish_tokens(
            mixed, resid, vectors, b_up_all[None], map_bkv.reshape(2, width), probe_cols, (w_out_all, w_up_all, w_down_all, pool_wk, pool_wv), head_dim)
        pooled = jnp.sum(jnp.where(on_head.T, every_head, 0.0).reshape(n_heads, n_heads, head_dim), axis=1)
        parts = lax.all_gather(jnp.concatenate([pooled, total, peak], axis=-1), 'tp', axis=0, tiled=False)
        parts = parts.reshape(n_images, tp_size // n_images, n_heads, head_dim + 2)
        pooled_all, total_all, peak_all = parts[..., :head_dim], parts[..., head_dim:head_dim + 1], parts[..., head_dim + 1:]
        share = jnp.exp(peak_all - jnp.max(peak_all, axis=1, keepdims=True))
        pooled_heads = (jnp.sum(pooled_all * share, axis=1) / jnp.sum(total_all * share, axis=1)).astype(jnp.bfloat16)
        return map_tail(pooled_heads, map_wo, map_bo, map_ln_gain, map_ln_bias, map_w_up, map_b_up, map_w_down, map_b_down)

    return jax.shard_map(local_program, mesh=mesh, in_specs=in_specs, out_specs=P('dp', None), check_vma=False)
```

```python
import functools

import jax
import jax.numpy as jnp
from jax import lax
from jax.experimental import pallas as pl
from jax.experimental.layout import Layout, with_layout_constraint
from jax.experimental.pallas import tpu as pltpu
from jax.sharding import PartitionSpec as P

LN_EPS = 1e-6
LOG2E = 1.4426950408889634
LANES = 128
BF16_MAX = 3.3895313892515355e38


def layer_norm(values, gain_vec, bias_vec):
    centered = values - jnp.mean(values, axis=-1, keepdims=True)
    variance = jnp.mean(centered * centered, axis=-1, keepdims=True)
    return centered * lax.rsqrt(variance + LN_EPS) * gain_vec + bias_vec


def row_major(values):
    return with_layout_constraint(values, Layout(major_to_minor=tuple(range(values.ndim))))


def round_up(size, multiple):
    return -(-size // multiple) * multiple


def attention_kernel(head_dim, chunk, *refs):
    out_ref, scores_a, scores_b, max_a, max_b, first_out, apart = refs[-7:]
    q_refs, k_refs, v_refs, v_last_refs = refs[:2], refs[2:6], refs[6:10], refs[10:14]
    part_keys = k_refs[0].shape[1]
    block = q_refs[0].shape[1]
    step = pl.program_id(0)
    exp_scale = head_dim ** -0.5 * LOG2E

    def score_chunk(keys_t, queries, rows, scores, running):
        part = lax.dot_general(keys_t, queries, (((0,), (0,)), ((), ())), preferred_element_type=jnp.float32)
        scores[rows, :] = part
        part_max = jnp.max(part.reshape(chunk // 8, 8, block), axis=0)
        return part_max if running is None else jnp.maximum(running, part_max)

    def mix_chunk(values, rows, scores, peak, total, mixed):
        weights = jnp.exp2((scores[rows, :] - peak) * exp_scale)
        part_total = jnp.sum(weights.reshape(chunk // 8, 8, block), axis=0)
        part_mixed = jnp.dot(values, weights.astype(jnp.bfloat16), preferred_element_type=jnp.float32)
        if total is None:
            return part_total, part_mixed
        return total + part_total, mixed + part_mixed

    def overlap(query_slot, score_buf, max_buf, v_parts, mix_buf, mix_max):
        running, total, mixed = None, None, None
        peak = jnp.max(mix_max[...], axis=0, keepdims=True)
        queries = q_refs[query_slot][...]
        for part, (k_ref, v_ref) in enumerate(zip(k_refs, v_parts)):
            for start in range(0, part_keys, chunk):
                rows = pl.ds(part * part_keys + start, chunk)
                running = score_chunk(k_ref[:, start:start + chunk], queries, rows, score_buf, running)
                total, mixed = mix_chunk(v_ref[:, start:start + chunk], rows, mix_buf, peak, total, mixed)
        max_buf[...] = running
        return mixed[:head_dim] / jnp.sum(total, axis=0, keepdims=True)

    def write(half, values_t):
        filled = jnp.concatenate([values_t, jnp.zeros((LANES - head_dim, block), jnp.float32)], axis=0)
        out_ref[half] = filled.T.astype(out_ref.dtype)

    @pl.when(step == 0)
    def _():
        apart[0] = 0
        scores_b[...] = jnp.zeros_like(scores_b)
        max_b[...] = jnp.zeros_like(max_b)
        first_out[...] = jnp.zeros_like(first_out)

    @pl.when(apart[0] == 0)
    def _():
        second = overlap(0, scores_a, max_a, v_last_refs, scores_b, max_b)
        write(0, first_out[...])
        write(1, second)

    @pl.when(step < pl.num_programs(0) - 1)
    def _():
        first_out[...] = overlap(1, scores_b, max_b, v_refs, scores_a, max_a)


def heads_attention(parts, head_dim, heads, place, stride, previous, n_out):
    first, count = heads
    n_part = parts[0].shape[1]
    block = n_part // 2
    per_head = n_part // block
    last = count * per_head - 1
    now = lambda i: first + jnp.minimum(i, last) // per_head
    before = lambda i: first + jnp.maximum(i - 1, 0) // per_head
    rows = round_up(head_dim, 16)
    whole = (rows, n_part)
    in_specs = [pl.BlockSpec((rows, block), lambda i: (3 * now(i), jnp.minimum(i, last) % per_head))] * 2
    in_specs += [pl.BlockSpec(whole, lambda i: (3 * now(i) + 1, 0))] * 4
    in_specs += [pl.BlockSpec(whole, lambda i: (3 * now(i) + 2, 0))] * 4
    in_specs += [pl.BlockSpec(whole, lambda i: (3 * before(i) + 2, 0))] * 4
    operands = [*parts[:2], *parts, *parts, *parts]
    aliases = {}
    if previous is not None:
        in_specs.append(pl.BlockSpec(memory_space=pl.ANY))
        operands.append(previous)
        aliases = {len(operands) - 1: 0}
    scored = count * 2 * n_part * 4 * n_part
    return pl.pallas_call(
        functools.partial(attention_kernel, head_dim, 256),
        grid=(last + 2,),
        out_shape=jax.ShapeDtypeStruct((2, n_part, n_out * LANES), jnp.bfloat16),
        in_specs=in_specs,
        out_specs=pl.BlockSpec((2, block, LANES), lambda i: (0, jnp.maximum(i - 1, 0) % per_head, place + stride * before(i))),
        scratch_shapes=[
            pltpu.VMEM((4 * n_part, block), jnp.float32),
            pltpu.VMEM((4 * n_part, block), jnp.float32),
            pltpu.VMEM((8, block), jnp.float32),
            pltpu.VMEM((8, block), jnp.float32),
            pltpu.VMEM((head_dim, block), jnp.float32),
            pltpu.SMEM((1,), jnp.int32),
        ],
        input_output_aliases=aliases,
        compiler_params=pltpu.CompilerParams(dimension_semantics=('arbitrary',), vmem_limit_bytes=40 * 1024 * 1024),
        cost_estimate=pl.CostEstimate(flops=4 * scored * LANES, bytes_accessed=8 * 1024 * 1024, transcendentals=scored),
        name='heads_attention',
    )(*operands)


def project_kernel(x_ref, gain_ref, shift_ref, weight_ref, bias_ref, out_ref):
    hidden = layer_norm(x_ref[...].astype(jnp.float32), gain_ref[...], shift_ref[...]).astype(jnp.bfloat16)
    product = lax.dot_general(weight_ref[...], hidden, (((1,), (1,)), ((), ())), preferred_element_type=jnp.float32)
    out_ref[...] = (product + bias_ref[...]).astype(out_ref.dtype)


def project_tokens(resid, gain, shift, weight, bias, block=512):
    n_own, width = resid.shape
    rows = weight.shape[0]
    fixed = lambda shape: pl.BlockSpec(shape, lambda i: (0, 0))
    return pl.pallas_call(
        project_kernel,
        grid=(n_own // block,),
        out_shape=jax.ShapeDtypeStruct((rows, n_own), jnp.bfloat16),
        in_specs=[pl.BlockSpec((block, width), lambda i: (i, 0)), fixed((1, width)), fixed((1, width)), fixed((rows, width)), fixed((rows, 1))],
        out_specs=pl.BlockSpec((rows, block), lambda i: (0, i)),
        compiler_params=pltpu.CompilerParams(dimension_semantics=('arbitrary',), vmem_limit_bytes=32 * 1024 * 1024),
        cost_estimate=pl.CostEstimate(flops=2 * n_own * width * rows, bytes_accessed=2 * (n_own * width + rows * width + rows * n_own), transcendentals=n_own),
        name='project_tokens',
    )(resid, gain[None], shift[None], weight, bias)


def split_three(values):
    high = lax.reduce_precision(jnp.clip(values, -BF16_MAX, BF16_MAX), 8, 7)
    middle = lax.reduce_precision(values - high, 8, 7)
    return [high.astype(jnp.bfloat16), middle.astype(jnp.bfloat16), (values - high - middle).astype(jnp.bfloat16)]


def join_three(parts):
    high, middle, low = (part.astype(jnp.float32) for part in parts)
    return high + middle + low


def finish_kernel(head_dim, up_chunk, mixed_ref, resid_a_ref, resid_b_ref, vec_ref, up_bias_ref, pool_bias_ref, probe_ref, w_out_hbm, w_up_hbm, w_down_hbm, wk_hbm, wv_hbm,
                  pooled_ref, total_ref, peak_ref, w_out, w_up, w_down, wk, wv, units, sems):
    step = pl.program_id(0)
    copies = [pltpu.make_async_copy(src, dst, sems.at[index]) for index, (src, dst) in enumerate(
        ((w_out_hbm, w_out), (w_up_hbm, w_up), (w_down_hbm, w_down), (wk_hbm, wk), (wv_hbm, wv)))]

    @pl.when(step == 0)
    def _():
        for copy in copies:
            copy.start()
        pooled_ref[...] = jnp.zeros_like(pooled_ref)
        total_ref[...] = jnp.zeros_like(total_ref)
        peak_ref[...] = jnp.full_like(peak_ref, -jnp.inf)

    def arrive(index):
        @pl.when(step == 0)
        def _():
            copies[index].wait()

    b_out, ln2_gain, ln2_bias, b_down, lnf_gain, lnf_bias = (vec_ref[index:index + 1, :] for index in range(6))
    arrive(0)
    attn_local = jnp.dot(mixed_ref[...], w_out[...], preferred_element_type=jnp.float32)
    resid = jnp.where(step < pl.num_programs(0) // 2, resid_a_ref[...].astype(jnp.float32), resid_b_ref[...].astype(jnp.float32))
    resid_one = (resid + attn_local + b_out).astype(jnp.bfloat16)
    hidden_two = layer_norm(resid_one.astype(jnp.float32), ln2_gain, ln2_bias).astype(jnp.bfloat16)
    arrive(1)
    n_units = w_up.shape[0]
    for start in range(0, n_units, up_chunk):
        cols = slice(start, min(start + up_chunk, n_units))
        pre_act = lax.dot_general(hidden_two, w_up[cols, :], (((1,), (1,)), ((), ())), preferred_element_type=jnp.float32) + up_bias_ref[:, cols]
        units[:, cols] = jax.nn.gelu(pre_act, approximate=True).astype(jnp.bfloat16)
    arrive(2)
    mlp_local = jnp.dot(units[...], w_down[...], preferred_element_type=jnp.float32)
    resid_two = (resid_one.astype(jnp.float32) + mlp_local + b_down).astype(jnp.bfloat16)
    encoded = layer_norm(resid_two.astype(jnp.float32), lnf_gain, lnf_bias).astype(jnp.bfloat16)
    arrive(3)
    keys = (jnp.dot(encoded, wk[...], preferred_element_type=jnp.float32) + pool_bias_ref[0:1, :]).astype(jnp.bfloat16)
    arrive(4)
    values = (jnp.dot(encoded, wv[...], preferred_element_type=jnp.float32) + pool_bias_ref[1:2, :]).astype(jnp.bfloat16)
    scores = lax.dot_general(probe_ref[...], keys, (((1,), (1,)), ((), ())), preferred_element_type=jnp.float32) * head_dim ** -0.5
    peak = jnp.maximum(peak_ref[...], jnp.max(scores, axis=-1, keepdims=True))
    weights = jnp.exp(scores - peak)
    keep = jnp.exp(peak_ref[...] - peak)
    total_ref[...] = total_ref[...] * keep + jnp.sum(weights, axis=-1, keepdims=True)
    pooled_ref[...] = pooled_ref[...] * keep + jnp.dot(weights.astype(jnp.bfloat16), values, preferred_element_type=jnp.float32)
    peak_ref[...] = peak


def finish_tokens(mixed, resid_parts, vectors, up_bias, pool_bias, probe, weights, head_dim, block=512):
    n_own, width = mixed.shape[0], resid_parts[0].shape[1]
    n_heads = probe.shape[0]
    per_part = n_own // 2 // block
    n_units = up_bias.shape[1]
    fixed = lambda shape: pl.BlockSpec(shape, lambda i: (0, 0))
    small = [vectors, up_bias, pool_bias, probe]
    return pl.pallas_call(
        functools.partial(finish_kernel, head_dim, 512),
        grid=(n_own // block,),
        out_shape=[jax.ShapeDtypeStruct((n_heads, columns), jnp.float32) for columns in (width, 1, 1)],
        in_specs=[pl.BlockSpec((block, mixed.shape[1]), lambda i: (i, 0)), pl.BlockSpec((block, width), lambda i: (jnp.minimum(i, per_part - 1), 0)), pl.BlockSpec((block, width), lambda i: (jnp.maximum(i - per_part, 0), 0))]
        + [fixed(array.shape) for array in small] + [pl.BlockSpec(memory_space=pl.ANY)] * len(weights),
        out_specs=[fixed((n_heads, columns)) for columns in (width, 1, 1)],
        scratch_shapes=[pltpu.VMEM(weight.shape, jnp.bfloat16) for weight in weights]
        + [pltpu.VMEM((block, n_units), jnp.bfloat16), pltpu.SemaphoreType.DMA((len(weights),))],
        compiler_params=pltpu.CompilerParams(dimension_semantics=('arbitrary',), vmem_limit_bytes=60 * 1024 * 1024),
        cost_estimate=pl.CostEstimate(flops=2 * n_own * sum(weight.size for weight in weights), bytes_accessed=40 * 1024 * 1024, transcendentals=n_own * n_units),
        name='finish_tokens',
    )(mixed, *resid_parts, *small, *weights)


def map_tail(pooled_heads, map_wo, map_bo, map_ln_gain, map_ln_bias, map_w_up, map_b_up, map_w_down, map_b_down):
    attn_vec = jnp.einsum('bhe,hed->bd', pooled_heads, map_wo, preferred_element_type=jnp.float32) + map_bo
    map_hidden = layer_norm(attn_vec, map_ln_gain, map_ln_bias).astype(jnp.bfloat16)
    map_act = jax.nn.gelu(jnp.dot(map_hidden, map_w_up, preferred_element_type=jnp.float32) + map_b_up, approximate=True).astype(jnp.bfloat16)
    return (attn_vec + jnp.dot(map_act, map_w_down, preferred_element_type=jnp.float32) + map_b_down).astype(jnp.bfloat16)


def solution(mesh):
    tp_size = mesh.shape['tp']
    in_specs = (P('dp', 'tp', None), P(), P(), P(None, None, 'tp', None), P(None, 'tp', None), P('tp', None, None), P(), P(), P(), P(None, 'tp'), P('tp'), P('tp', None)) + (P(),) * 16
    partner = [(device, device ^ 1) for device in range(tp_size)]

    def local_program(tokens, ln1_gain, ln1_bias, w_qkv, b_qkv, w_out, b_out, ln2_gain, ln2_bias, w_up, b_up, w_down, b_down, lnf_gain, lnf_bias, probe_vec, map_wq, map_bq, map_wkv, map_bkv, map_wo, map_bo, map_ln_gain, map_ln_bias, map_w_up, map_b_up, map_w_down, map_b_down):
        n_images, run, width = tokens.shape
        groups, head_dim = w_qkv.shape[2:]
        n_heads = groups * tp_size
        hidden_units = w_up.shape[1]
        own = n_images * run

        pieces = tokens.reshape(tp_size, 2, own // tp_size // 2, width)

        def send(piece):
            return row_major(lax.all_to_all(row_major(pieces[:, piece]), 'tp', split_axis=0, concat_axis=0, tiled=True).reshape(own // 2, width))

        resid_a, resid_b = send(0), send(1)

        rows_padded = round_up(head_dim, 16)
        shards = []
        for group in range(groups):
            rows = jnp.transpose(w_qkv[:, :, group], (1, 2, 0))
            bias_row = jnp.concatenate(split_three(b_qkv[:, group].reshape(3 * head_dim)))
            bias_row = jnp.pad(bias_row, (0, width - bias_row.shape[0]))[None]
            extra = jnp.pad(bias_row, ((0, rows_padded - head_dim - 1), (0, 0)))
            none = jnp.zeros_like(extra)
            shards.append(jnp.concatenate([rows[0], none, rows[1], none, rows[2], extra], axis=0))
        padded = round_up(hidden_units, 32)
        w_up_t = jnp.pad(w_up.T, ((0, padded - hidden_units), (0, 0)))
        high, middle, low = split_three(b_up)
        up_rows = jnp.stack([jnp.pad(jnp.concatenate([high, middle]), (0, width - 2 * hidden_units)), jnp.pad(low, (0, width - hidden_units))])
        w_down_p = jnp.pad(jnp.concatenate([w_down, up_rows], axis=0), ((0, padded - hidden_units - 2), (0, 0)))

        gathered = [lax.all_gather(shards[0], 'tp', axis=0, tiled=True)]
        probe_q = (jnp.dot(probe_vec[None], map_wq.reshape(width, width), preferred_element_type=jnp.float32)[0] + map_bq.reshape(width)).astype(jnp.bfloat16)
        head_of = jnp.arange(width) // head_dim
        on_head = head_of[:, None] == jnp.arange(n_heads)[None]
        probe_cols = jnp.where(on_head.T, probe_q[None], jnp.zeros((), jnp.bfloat16))
        pool_wk, pool_wv = (row_major(map_wkv[:, index].reshape(width, width)) for index in range(2))
        vectors = jnp.stack([b_out, ln2_gain, ln2_bias, b_down, lnf_gain, lnf_bias])
        w_out_p = jnp.pad(w_out, ((0, 0), (0, LANES - head_dim), (0, 0))).reshape(groups * LANES, width)
        def project(group_rows, part):
            bias_row = group_rows.reshape(tp_size, 3 * rows_padded, width)[:, 2 * rows_padded + head_dim, :9 * head_dim]
            bias_row = bias_row.reshape(tp_size, 3, 3, head_dim)
            bias = join_three([bias_row[:, term] for term in range(3)])
            bias = jnp.pad(bias, ((0, 0), (0, 0), (0, rows_padded - head_dim))).reshape(-1, 1)
            return project_tokens(part, ln1_gain, ln1_bias, group_rows, bias)

        def swap(part):
            return lax.ppermute(part, 'tp', partner)

        first_a = project(gathered[0], resid_a)
        far_a = swap(first_a)
        first_b = project(gathered[0], resid_b)
        far_a_later, later_parts, later, w_out_p, w_up_t, w_down_p, probe_cols, pool_wk, pool_wv, vectors = lax.optimization_barrier(
            (far_a, (resid_a, resid_b), shards[1:], w_out_p, w_up_t, w_down_p, probe_cols, pool_wk, pool_wv, vectors))
        gathered += [lax.all_gather(shard, 'tp', axis=0, tiled=True) for shard in later]
        w_out_all = lax.all_gather(w_out_p, 'tp', axis=0, tiled=True)
        w_up_all = lax.all_gather(w_up_t, 'tp', axis=0, tiled=True)
        w_down_all = lax.all_gather(w_down_p, 'tp', axis=0, tiled=True)

        half = tp_size // 2
        first_group = [first_a, first_b, far_a, swap(first_b)]
        mixed = heads_attention(first_group, head_dim, (0, half), 0, groups, None, n_heads)
        mixed, later_parts, gathered[1] = lax.optimization_barrier((mixed, later_parts, gathered[1]))
        second_group = [project(gathered[1], part) for part in later_parts]
        second_group += [swap(part) for part in second_group]
        mixed = heads_attention([first_a, first_b, far_a_later, first_group[3]], head_dim, (half, half), 0, groups, mixed, n_heads)
        mixed = heads_attention(second_group, head_dim, (0, tp_size), 1, groups, mixed, n_heads)

        bias_rows = w_down_all.reshape(tp_size, padded, width)[:, hidden_units:hidden_units + 2]
        b_up_all = join_three([bias_rows[:, 0, :hidden_units], bias_rows[:, 0, hidden_units:2 * hidden_units], bias_rows[:, 1, :hidden_units]])
        b_up_all = jnp.pad(b_up_all, ((0, 0), (0, padded - hidden_units))).reshape(tp_size * padded)
        every_head, total, peak = finish_tokens(
            mixed.reshape(own, n_heads * LANES), later_parts, vectors, b_up_all[None], map_bkv.reshape(2, width), probe_cols, (w_out_all, w_up_all, w_down_all, pool_wk, pool_wv), head_dim)
        pooled = jnp.sum(jnp.where(on_head.T, every_head, 0.0).reshape(n_heads, n_heads, head_dim), axis=1)
        parts = lax.all_gather(jnp.concatenate([pooled, total, peak], axis=-1), 'tp', axis=0, tiled=False)
        parts = parts.reshape(n_images, tp_size // n_images, n_heads, head_dim + 2)
        pooled_all, total_all, peak_all = parts[..., :head_dim], parts[..., head_dim:head_dim + 1], parts[..., head_dim + 1:]
        share = jnp.exp(peak_all - jnp.max(peak_all, axis=1, keepdims=True))
        pooled_heads = (jnp.sum(pooled_all * share, axis=1) / jnp.sum(total_all * share, axis=1)).astype(jnp.bfloat16)
        return map_tail(pooled_heads, map_wo, map_bo, map_ln_gain, map_ln_bias, map_w_up, map_b_up, map_w_down, map_b_down)

    return jax.shard_map(local_program, mesh=mesh, in_specs=in_specs, out_specs=P('dp', None), check_vma=False)
```

```python
import functools

import jax
import jax.numpy as jnp
from jax import lax
from jax.experimental import pallas as pl
from jax.experimental.layout import Layout, with_layout_constraint
from jax.experimental.pallas import tpu as pltpu
from jax.sharding import PartitionSpec as P

LN_EPS = 1e-6
LOG2E = 1.4426950408889634
LANES = 128
BF16_MAX = 3.3895313892515355e38


def layer_norm(values, gain_vec, bias_vec):
    centered = values - jnp.mean(values, axis=-1, keepdims=True)
    variance = jnp.mean(centered * centered, axis=-1, keepdims=True)
    return centered * lax.rsqrt(variance + LN_EPS) * gain_vec + bias_vec


def row_major(values):
    return with_layout_constraint(values, Layout(major_to_minor=tuple(range(values.ndim))))


def round_up(size, multiple):
    return -(-size // multiple) * multiple


def attention_kernel(head_dim, chunk, *refs):
    out_ref, scores_a, scores_b, max_a, max_b, first_out, apart = refs[-7:]
    q_refs, k_refs, v_refs, v_last_refs = refs[:2], refs[2:6], refs[6:10], refs[10:14]
    part_keys = k_refs[0].shape[1]
    block = q_refs[0].shape[1]
    step = pl.program_id(0)
    exp_scale = head_dim ** -0.5 * LOG2E

    def score_chunk(keys_t, queries, rows, scores, running):
        part = lax.dot_general(keys_t, queries, (((0,), (0,)), ((), ())), preferred_element_type=jnp.float32)
        scores[rows, :] = part
        part_max = jnp.max(part.reshape(chunk // 8, 8, block), axis=0)
        return part_max if running is None else jnp.maximum(running, part_max)

    def mix_chunk(values, rows, scores, peak, total, mixed):
        weights = jnp.exp2((scores[rows, :] - peak) * exp_scale)
        part_total = jnp.sum(weights.reshape(chunk // 8, 8, block), axis=0)
        part_mixed = jnp.dot(values, weights.astype(jnp.bfloat16), preferred_element_type=jnp.float32)
        if total is None:
            return part_total, part_mixed
        return total + part_total, mixed + part_mixed

    def overlap(query_slot, score_buf, max_buf, v_parts, mix_buf, mix_max):
        running, total, mixed = None, None, None
        peak = jnp.max(mix_max[...], axis=0, keepdims=True)
        queries = q_refs[query_slot][...]
        for part, (k_ref, v_ref) in enumerate(zip(k_refs, v_parts)):
            for start in range(0, part_keys, chunk):
                rows = pl.ds(part * part_keys + start, chunk)
                running = score_chunk(k_ref[:, start:start + chunk], queries, rows, score_buf, running)
                total, mixed = mix_chunk(v_ref[:, start:start + chunk], rows, mix_buf, peak, total, mixed)
        max_buf[...] = running
        return mixed[:head_dim] / jnp.sum(total, axis=0, keepdims=True)

    def write(half, values_t):
        filled = jnp.concatenate([values_t, jnp.zeros((LANES - head_dim, block), jnp.float32)], axis=0)
        out_ref[half] = filled.T.astype(out_ref.dtype)

    @pl.when(step == 0)
    def _():
        apart[0] = 0
        scores_b[...] = jnp.zeros_like(scores_b)
        max_b[...] = jnp.zeros_like(max_b)
        first_out[...] = jnp.zeros_like(first_out)

    @pl.when(apart[0] == 0)
    def _():
        second = overlap(0, scores_a, max_a, v_last_refs, scores_b, max_b)
        write(0, first_out[...])
        write(1, second)

    @pl.when(step < pl.num_programs(0) - 1)
    def _():
        first_out[...] = overlap(1, scores_b, max_b, v_refs, scores_a, max_a)


def heads_attention(parts, head_dim, heads, place, stride, previous, n_out):
    first, count = heads
    n_part = parts[0].shape[1]
    block = n_part // 2
    per_head = n_part // block
    last = count * per_head - 1
    now = lambda i: first + jnp.minimum(i, last) // per_head
    before = lambda i: first + jnp.maximum(i - 1, 0) // per_head
    rows = round_up(head_dim, 16)
    whole = (rows, n_part)
    in_specs = [pl.BlockSpec((rows, block), lambda i: (3 * now(i), jnp.minimum(i, last) % per_head))] * 2
    in_specs += [pl.BlockSpec(whole, lambda i: (3 * now(i) + 1, 0))] * 4
    in_specs += [pl.BlockSpec(whole, lambda i: (3 * now(i) + 2, 0))] * 4
    in_specs += [pl.BlockSpec(whole, lambda i: (3 * before(i) + 2, 0))] * 4
    operands = [*parts[:2], *parts, *parts, *parts]
    aliases = {}
    if previous is not None:
        in_specs.append(pl.BlockSpec(memory_space=pl.ANY))
        operands.append(previous)
        aliases = {len(operands) - 1: 0}
    scored = count * 2 * n_part * 4 * n_part
    return pl.pallas_call(
        functools.partial(attention_kernel, head_dim, 256),
        grid=(last + 2,),
        out_shape=jax.ShapeDtypeStruct((2, n_part, n_out * LANES), jnp.bfloat16),
        in_specs=in_specs,
        out_specs=pl.BlockSpec((2, block, LANES), lambda i: (0, jnp.maximum(i - 1, 0) % per_head, place + stride * before(i))),
        scratch_shapes=[
            pltpu.VMEM((4 * n_part, block), jnp.float32),
            pltpu.VMEM((4 * n_part, block), jnp.float32),
            pltpu.VMEM((8, block), jnp.float32),
            pltpu.VMEM((8, block), jnp.float32),
            pltpu.VMEM((head_dim, block), jnp.float32),
            pltpu.SMEM((1,), jnp.int32),
        ],
        input_output_aliases=aliases,
        compiler_params=pltpu.CompilerParams(dimension_semantics=('arbitrary',), vmem_limit_bytes=40 * 1024 * 1024),
        cost_estimate=pl.CostEstimate(flops=4 * scored * LANES, bytes_accessed=8 * 1024 * 1024, transcendentals=scored),
        name='heads_attention',
    )(*operands)


def project_kernel(x_ref, gain_ref, shift_ref, weight_ref, bias_ref, out_ref):
    hidden = layer_norm(x_ref[...].astype(jnp.float32), gain_ref[...], shift_ref[...]).astype(jnp.bfloat16)
    product = lax.dot_general(weight_ref[...], hidden, (((1,), (1,)), ((), ())), preferred_element_type=jnp.float32)
    out_ref[...] = (product + bias_ref[...]).astype(out_ref.dtype)


def project_tokens(resid, part, gain, shift, weight, bias, block=512):
    n_own, width = resid.shape[0] // 2, resid.shape[1]
    first = part * (n_own // block)
    rows = weight.shape[0]
    fixed = lambda shape: pl.BlockSpec(shape, lambda i: (0, 0))
    return pl.pallas_call(
        project_kernel,
        grid=(n_own // block,),
        out_shape=jax.ShapeDtypeStruct((rows, n_own), jnp.bfloat16),
        in_specs=[pl.BlockSpec((block, width), lambda i: (first + i, 0)), fixed((1, width)), fixed((1, width)), fixed((rows, width)), fixed((rows, 1))],
        out_specs=pl.BlockSpec((rows, block), lambda i: (0, i)),
        compiler_params=pltpu.CompilerParams(dimension_semantics=('arbitrary',), vmem_limit_bytes=32 * 1024 * 1024),
        cost_estimate=pl.CostEstimate(flops=2 * n_own * width * rows, bytes_accessed=2 * (n_own * width + rows * width + rows * n_own), transcendentals=n_own),
        name='project_tokens',
    )(resid, gain[None], shift[None], weight, bias)


def split_three(values):
    high = lax.reduce_precision(jnp.clip(values, -BF16_MAX, BF16_MAX), 8, 7)
    middle = lax.reduce_precision(values - high, 8, 7)
    return [high.astype(jnp.bfloat16), middle.astype(jnp.bfloat16), (values - high - middle).astype(jnp.bfloat16)]


def join_three(parts):
    high, middle, low = (part.astype(jnp.float32) for part in parts)
    return high + middle + low


def finish_kernel(head_dim, up_chunk, mixed_ref, resid_ref, vec_ref, up_bias_ref, pool_bias_ref, probe_ref, w_out_hbm, w_up_hbm, w_down_hbm, wk_hbm, wv_hbm,
                  pooled_ref, total_ref, peak_ref, w_out, w_up, w_down, wk, wv, units, sems):
    step = pl.program_id(0)
    copies = [pltpu.make_async_copy(src, dst, sems.at[index]) for index, (src, dst) in enumerate(
        ((w_out_hbm, w_out), (w_up_hbm, w_up), (w_down_hbm, w_down), (wk_hbm, wk), (wv_hbm, wv)))]

    @pl.when(step == 0)
    def _():
        for copy in copies:
            copy.start()
        pooled_ref[...] = jnp.zeros_like(pooled_ref)
        total_ref[...] = jnp.zeros_like(total_ref)
        peak_ref[...] = jnp.full_like(peak_ref, -jnp.inf)

    def arrive(index):
        @pl.when(step == 0)
        def _():
            copies[index].wait()

    b_out, ln2_gain, ln2_bias, b_down, lnf_gain, lnf_bias = (vec_ref[index:index + 1, :] for index in range(6))
    arrive(0)
    attn_local = jnp.dot(mixed_ref[...], w_out[...], preferred_element_type=jnp.float32)
    resid_one = (resid_ref[...].astype(jnp.float32) + attn_local + b_out).astype(jnp.bfloat16)
    hidden_two = layer_norm(resid_one.astype(jnp.float32), ln2_gain, ln2_bias).astype(jnp.bfloat16)
    arrive(1)
    n_units = w_up.shape[0]
    for start in range(0, n_units, up_chunk):
        cols = slice(start, min(start + up_chunk, n_units))
        pre_act = lax.dot_general(hidden_two, w_up[cols, :], (((1,), (1,)), ((), ())), preferred_element_type=jnp.float32) + up_bias_ref[:, cols]
        units[:, cols] = jax.nn.gelu(pre_act, approximate=True).astype(jnp.bfloat16)
    arrive(2)
    mlp_local = jnp.dot(units[...], w_down[...], preferred_element_type=jnp.float32)
    resid_two = (resid_one.astype(jnp.float32) + mlp_local + b_down).astype(jnp.bfloat16)
    encoded = layer_norm(resid_two.astype(jnp.float32), lnf_gain, lnf_bias).astype(jnp.bfloat16)
    arrive(3)
    keys = (jnp.dot(encoded, wk[...], preferred_element_type=jnp.float32) + pool_bias_ref[0:1, :]).astype(jnp.bfloat16)
    arrive(4)
    values = (jnp.dot(encoded, wv[...], preferred_element_type=jnp.float32) + pool_bias_ref[1:2, :]).astype(jnp.bfloat16)
    scores = lax.dot_general(probe_ref[...], keys, (((1,), (1,)), ((), ())), preferred_element_type=jnp.float32) * head_dim ** -0.5
    peak = jnp.maximum(peak_ref[...], jnp.max(scores, axis=-1, keepdims=True))
    weights = jnp.exp(scores - peak)
    keep = jnp.exp(peak_ref[...] - peak)
    total_ref[...] = total_ref[...] * keep + jnp.sum(weights, axis=-1, keepdims=True)
    pooled_ref[...] = pooled_ref[...] * keep + jnp.dot(weights.astype(jnp.bfloat16), values, preferred_element_type=jnp.float32)
    peak_ref[...] = peak


def finish_tokens(mixed, resid, vectors, up_bias, pool_bias, probe, weights, head_dim, block=512):
    n_own, width = resid.shape
    n_heads = probe.shape[0]
    n_units = up_bias.shape[1]
    fixed = lambda shape: pl.BlockSpec(shape, lambda i: (0, 0))
    small = [vectors, up_bias, pool_bias, probe]
    return pl.pallas_call(
        functools.partial(finish_kernel, head_dim, 512),
        grid=(n_own // block,),
        out_shape=[jax.ShapeDtypeStruct((n_heads, columns), jnp.float32) for columns in (width, 1, 1)],
        in_specs=[pl.BlockSpec((block, mixed.shape[1]), lambda i: (i, 0)), pl.BlockSpec((block, width), lambda i: (i, 0))]
        + [fixed(array.shape) for array in small] + [pl.BlockSpec(memory_space=pl.ANY)] * len(weights),
        out_specs=[fixed((n_heads, columns)) for columns in (width, 1, 1)],
        scratch_shapes=[pltpu.VMEM(weight.shape, jnp.bfloat16) for weight in weights]
        + [pltpu.VMEM((block, n_units), jnp.bfloat16), pltpu.SemaphoreType.DMA((len(weights),))],
        compiler_params=pltpu.CompilerParams(dimension_semantics=('arbitrary',), vmem_limit_bytes=60 * 1024 * 1024),
        cost_estimate=pl.CostEstimate(flops=2 * n_own * sum(weight.size for weight in weights), bytes_accessed=40 * 1024 * 1024, transcendentals=n_own * n_units),
        name='finish_tokens',
    )(mixed, resid, *small, *weights)


def map_tail(pooled_heads, map_wo, map_bo, map_ln_gain, map_ln_bias, map_w_up, map_b_up, map_w_down, map_b_down):
    attn_vec = jnp.einsum('bhe,hed->bd', pooled_heads, map_wo, preferred_element_type=jnp.float32) + map_bo
    map_hidden = layer_norm(attn_vec, map_ln_gain, map_ln_bias).astype(jnp.bfloat16)
    map_act = jax.nn.gelu(jnp.dot(map_hidden, map_w_up, preferred_element_type=jnp.float32) + map_b_up, approximate=True).astype(jnp.bfloat16)
    return (attn_vec + jnp.dot(map_act, map_w_down, preferred_element_type=jnp.float32) + map_b_down).astype(jnp.bfloat16)


def solution(mesh):
    tp_size = mesh.shape['tp']
    in_specs = (P('dp', 'tp', None), P(), P(), P(None, None, 'tp', None), P(None, 'tp', None), P('tp', None, None), P(), P(), P(), P(None, 'tp'), P('tp'), P('tp', None)) + (P(),) * 16
    partner = [(device, device ^ 1) for device in range(tp_size)]

    def local_program(tokens, ln1_gain, ln1_bias, w_qkv, b_qkv, w_out, b_out, ln2_gain, ln2_bias, w_up, b_up, w_down, b_down, lnf_gain, lnf_bias, probe_vec, map_wq, map_bq, map_wkv, map_bkv, map_wo, map_bo, map_ln_gain, map_ln_bias, map_w_up, map_b_up, map_w_down, map_b_down):
        n_images, run, width = tokens.shape
        groups, head_dim = w_qkv.shape[2:]
        n_heads = groups * tp_size
        hidden_units = w_up.shape[1]
        own = n_images * run

        resid = row_major(lax.all_to_all(row_major(tokens.reshape(tp_size, own // tp_size, width)), 'tp', split_axis=0, concat_axis=0, tiled=True).reshape(own, width))

        rows_padded = round_up(head_dim, 16)
        shards = []
        for group in range(groups):
            rows = jnp.transpose(w_qkv[:, :, group], (1, 2, 0))
            bias_row = jnp.concatenate(split_three(b_qkv[:, group].reshape(3 * head_dim)))
            bias_row = jnp.pad(bias_row, (0, width - bias_row.shape[0]))[None]
            extra = jnp.pad(bias_row, ((0, rows_padded - head_dim - 1), (0, 0)))
            none = jnp.zeros_like(extra)
            shards.append(jnp.concatenate([rows[0], none, rows[1], none, rows[2], extra], axis=0))
        padded = round_up(hidden_units, 32)
        w_up_t = jnp.pad(w_up.T, ((0, padded - hidden_units), (0, 0)))
        high, middle, low = split_three(b_up)
        up_rows = jnp.stack([jnp.pad(jnp.concatenate([high, middle]), (0, width - 2 * hidden_units)), jnp.pad(low, (0, width - hidden_units))])
        w_down_p = jnp.pad(jnp.concatenate([w_down, up_rows], axis=0), ((0, padded - hidden_units - 2), (0, 0)))

        gathered = [lax.all_gather(shards[0], 'tp', axis=0, tiled=True)]
        probe_q = (jnp.dot(probe_vec[None], map_wq.reshape(width, width), preferred_element_type=jnp.float32)[0] + map_bq.reshape(width)).astype(jnp.bfloat16)
        head_of = jnp.arange(width) // head_dim
        on_head = head_of[:, None] == jnp.arange(n_heads)[None]
        probe_cols = jnp.where(on_head.T, probe_q[None], jnp.zeros((), jnp.bfloat16))
        pool_wk, pool_wv = (row_major(map_wkv[:, index].reshape(width, width)) for index in range(2))
        vectors = jnp.stack([b_out, ln2_gain, ln2_bias, b_down, lnf_gain, lnf_bias])
        w_out_p = jnp.pad(w_out, ((0, 0), (0, LANES - head_dim), (0, 0))).reshape(groups * LANES, width)
        resid, later, w_out_p, w_up_t, w_down_p, probe_cols, pool_wk, pool_wv, vectors, pool_bias = lax.optimization_barrier(
            (resid, shards[1:], w_out_p, w_up_t, w_down_p, probe_cols, pool_wk, pool_wv, vectors, map_bkv.reshape(2, width)))
        gathered += [lax.all_gather(shard, 'tp', axis=0, tiled=True) for shard in later]
        w_out_all = lax.all_gather(w_out_p, 'tp', axis=0, tiled=True)
        w_up_all = lax.all_gather(w_up_t, 'tp', axis=0, tiled=True)
        w_down_all = lax.all_gather(w_down_p, 'tp', axis=0, tiled=True)

        def projections(group_rows, resid):
            bias_row = group_rows.reshape(tp_size, 3 * rows_padded, width)[:, 2 * rows_padded + head_dim, :9 * head_dim]
            bias_row = bias_row.reshape(tp_size, 3, 3, head_dim)
            bias = join_three([bias_row[:, term] for term in range(3)])
            bias = jnp.pad(bias, ((0, 0), (0, 0), (0, rows_padded - head_dim))).reshape(-1, 1)
            first = project_tokens(resid, 0, ln1_gain, ln1_bias, group_rows, bias)
            second = project_tokens(resid, 1, ln1_gain, ln1_bias, group_rows, bias)
            return [first, second, lax.ppermute(first, 'tp', partner), lax.ppermute(second, 'tp', partner)]

        half = tp_size // 2
        first_group = projections(gathered[0], resid)
        mixed = heads_attention(first_group, head_dim, (0, half), 0, groups, None, n_heads)
        mixed, resid, gathered[1] = lax.optimization_barrier((mixed, resid, gathered[1]))
        second_group = projections(gathered[1], resid)
        mixed = heads_attention(first_group, head_dim, (half, half), 0, groups, mixed, n_heads)
        mixed = heads_attention(second_group, head_dim, (0, tp_size), 1, groups, mixed, n_heads)

        bias_rows = w_down_all.reshape(tp_size, padded, width)[:, hidden_units:hidden_units + 2]
        b_up_all = join_three([bias_rows[:, 0, :hidden_units], bias_rows[:, 0, hidden_units:2 * hidden_units], bias_rows[:, 1, :hidden_units]])
        b_up_all = jnp.pad(b_up_all, ((0, 0), (0, padded - hidden_units))).reshape(tp_size * padded)
        every_head, total, peak = finish_tokens(
            mixed.reshape(own, n_heads * LANES), resid, vectors, b_up_all[None], pool_bias, probe_cols, (w_out_all, w_up_all, w_down_all, pool_wk, pool_wv), head_dim)
        pooled = jnp.sum(jnp.where(on_head.T, every_head, 0.0).reshape(n_heads, n_heads, head_dim), axis=1)
        parts = lax.all_gather(jnp.concatenate([pooled, total, peak], axis=-1), 'tp', axis=0, tiled=False)
        parts = parts.reshape(n_images, tp_size // n_images, n_heads, head_dim + 2)
        pooled_all, total_all, peak_all = parts[..., :head_dim], parts[..., head_dim:head_dim + 1], parts[..., head_dim + 1:]
        share = jnp.exp(peak_all - jnp.max(peak_all, axis=1, keepdims=True))
        pooled_heads = (jnp.sum(pooled_all * share, axis=1) / jnp.sum(total_all * share, axis=1)).astype(jnp.bfloat16)
        return map_tail(pooled_heads, map_wo, map_bo, map_ln_gain, map_ln_bias, map_w_up, map_b_up, map_w_down, map_b_down)

    return jax.shard_map(local_program, mesh=mesh, in_specs=in_specs, out_specs=P('dp', None), check_vma=False)
```

```python
import functools

import jax
import jax.numpy as jnp
from jax import lax
from jax.experimental import pallas as pl
from jax.experimental.layout import Layout, with_layout_constraint
from jax.experimental.pallas import tpu as pltpu
from jax.sharding import PartitionSpec as P

LN_EPS = 1e-6
LOG2E = 1.4426950408889634
LANES = 128
BF16_MAX = 3.3895313892515355e38


def layer_norm(values, gain_vec, bias_vec):
    centered = values - jnp.mean(values, axis=-1, keepdims=True)
    variance = jnp.mean(centered * centered, axis=-1, keepdims=True)
    return centered * lax.rsqrt(variance + LN_EPS) * gain_vec + bias_vec


def row_major(values):
    return with_layout_constraint(values, Layout(major_to_minor=tuple(range(values.ndim))))


def round_up(size, multiple):
    return -(-size // multiple) * multiple


def attention_kernel(head_dim, chunk, *refs):
    out_ref, scores_a, scores_b, max_a, max_b, first_out, apart = refs[-7:]
    q_refs, k_refs, v_refs, v_last_refs = refs[:2], refs[2:6], refs[6:10], refs[10:14]
    part_keys = k_refs[0].shape[1]
    block = q_refs[0].shape[1]
    step = pl.program_id(0)
    exp_scale = head_dim ** -0.5 * LOG2E

    def score_chunk(keys_t, queries, rows, scores, running):
        part = lax.dot_general(keys_t, queries, (((0,), (0,)), ((), ())), preferred_element_type=jnp.float32)
        scores[rows, :] = part
        part_max = jnp.max(part.reshape(chunk // 8, 8, block), axis=0)
        return part_max if running is None else jnp.maximum(running, part_max)

    def mix_chunk(values, rows, scores, peak, total, mixed):
        weights = jnp.exp2((scores[rows, :] - peak) * exp_scale)
        part_total = jnp.sum(weights.reshape(chunk // 8, 8, block), axis=0)
        part_mixed = jnp.dot(values, weights.astype(jnp.bfloat16), preferred_element_type=jnp.float32)
        if total is None:
            return part_total, part_mixed
        return total + part_total, mixed + part_mixed

    def overlap(query_slot, score_buf, max_buf, v_parts, mix_buf, mix_max):
        running, total, mixed = None, None, None
        peak = jnp.max(mix_max[...], axis=0, keepdims=True)
        queries = q_refs[query_slot][...]
        for part, (k_ref, v_ref) in enumerate(zip(k_refs, v_parts)):
            for start in range(0, part_keys, chunk):
                rows = pl.ds(part * part_keys + start, chunk)
                running = score_chunk(k_ref[:, start:start + chunk], queries, rows, score_buf, running)
                total, mixed = mix_chunk(v_ref[:, start:start + chunk], rows, mix_buf, peak, total, mixed)
        max_buf[...] = running
        return mixed[:head_dim] / jnp.sum(total, axis=0, keepdims=True)

    def write(half, values_t):
        filled = jnp.concatenate([values_t, jnp.zeros((LANES - head_dim, block), jnp.float32)], axis=0)
        out_ref[half] = filled.T.astype(out_ref.dtype)

    @pl.when(step == 0)
    def _():
        apart[0] = 0
        max_b[...] = jnp.zeros_like(max_b)
        first_out[...] = jnp.zeros_like(first_out)

    @pl.when(apart[0] == 0)
    def _():
        second = overlap(0, scores_a, max_a, v_last_refs, scores_b, max_b)
        write(0, first_out[...])
        write(1, second)

    @pl.when(step < pl.num_programs(0) - 1)
    def _():
        first_out[...] = overlap(1, scores_b, max_b, v_refs, scores_a, max_a)


def heads_attention(parts, head_dim, heads, place, stride, previous, n_out):
    first, count = heads
    n_part = parts[0].shape[1]
    block = n_part // 2
    per_head = n_part // block
    last = count * per_head - 1
    now = lambda i: first + jnp.minimum(i, last) // per_head
    before = lambda i: first + jnp.maximum(i - 1, 0) // per_head
    rows = round_up(head_dim, 16)
    whole = (rows, n_part)
    in_specs = [pl.BlockSpec((rows, block), lambda i: (3 * now(i), jnp.minimum(i, last) % per_head))] * 2
    in_specs += [pl.BlockSpec(whole, lambda i: (3 * now(i) + 1, 0))] * 4
    in_specs += [pl.BlockSpec(whole, lambda i: (3 * now(i) + 2, 0))] * 4
    in_specs += [pl.BlockSpec(whole, lambda i: (3 * before(i) + 2, 0))] * 4
    operands = [*parts[:2], *parts, *parts, *parts]
    aliases = {}
    if previous is not None:
        in_specs.append(pl.BlockSpec(memory_space=pl.ANY))
        operands.append(previous)
        aliases = {len(operands) - 1: 0}
    scored = count * 2 * n_part * 4 * n_part
    return pl.pallas_call(
        functools.partial(attention_kernel, head_dim, 256),
        grid=(last + 2,),
        out_shape=jax.ShapeDtypeStruct((2, n_part, n_out * LANES), jnp.bfloat16),
        in_specs=in_specs,
        out_specs=pl.BlockSpec((2, block, LANES), lambda i: (0, jnp.maximum(i - 1, 0) % per_head, place + stride * before(i))),
        scratch_shapes=[
            pltpu.VMEM((4 * n_part, block), jnp.float32),
            pltpu.VMEM((4 * n_part, block), jnp.float32),
            pltpu.VMEM((8, block), jnp.float32),
            pltpu.VMEM((8, block), jnp.float32),
            pltpu.VMEM((head_dim, block), jnp.float32),
            pltpu.SMEM((1,), jnp.int32),
        ],
        input_output_aliases=aliases,
        compiler_params=pltpu.CompilerParams(dimension_semantics=('arbitrary',), vmem_limit_bytes=60 * 1024 * 1024),
        cost_estimate=pl.CostEstimate(flops=4 * scored * LANES, bytes_accessed=8 * 1024 * 1024, transcendentals=scored),
        name='heads_attention',
    )(*operands)


def project_kernel(x_ref, gain_ref, shift_ref, weight_ref, bias_ref, out_ref):
    hidden = layer_norm(x_ref[...].astype(jnp.float32), gain_ref[...], shift_ref[...]).astype(jnp.bfloat16)
    product = lax.dot_general(weight_ref[...], hidden, (((1,), (1,)), ((), ())), preferred_element_type=jnp.float32)
    out_ref[...] = (product + bias_ref[...]).astype(out_ref.dtype)


def project_tokens(resid, part, gain, shift, weight, bias, block=512):
    n_own, width = resid.shape[0] // 2, resid.shape[1]
    first = part * (n_own // block)
    rows = weight.shape[0]
    fixed = lambda shape: pl.BlockSpec(shape, lambda i: (0, 0))
    return pl.pallas_call(
        project_kernel,
        grid=(n_own // block,),
        out_shape=jax.ShapeDtypeStruct((rows, n_own), jnp.bfloat16),
        in_specs=[pl.BlockSpec((block, width), lambda i: (first + i, 0)), fixed((1, width)), fixed((1, width)), fixed((rows, width)), fixed((rows, 1))],
        out_specs=pl.BlockSpec((rows, block), lambda i: (0, i)),
        compiler_params=pltpu.CompilerParams(dimension_semantics=('arbitrary',), vmem_limit_bytes=60 * 1024 * 1024),
        cost_estimate=pl.CostEstimate(flops=2 * n_own * width * rows, bytes_accessed=2 * (n_own * width + rows * width + rows * n_own), transcendentals=n_own),
        name='project_tokens',
    )(resid, gain[None], shift[None], weight, bias)


def split_three(values):
    high = lax.reduce_precision(jnp.clip(values, -BF16_MAX, BF16_MAX), 8, 7)
    middle = lax.reduce_precision(values - high, 8, 7)
    return [high.astype(jnp.bfloat16), middle.astype(jnp.bfloat16), (values - high - middle).astype(jnp.bfloat16)]


def join_three(parts):
    high, middle, low = (part.astype(jnp.float32) for part in parts)
    return high + middle + low


def finish_kernel(head_dim, up_chunk, mixed_ref, resid_ref, vec_ref, up_bias_ref, pool_bias_ref, probe_ref, w_out_hbm, w_up_hbm, w_down_hbm, wk_hbm, wv_hbm,
                  pooled_ref, total_ref, peak_ref, w_out, w_up, w_down, wk, wv, units, sems):
    step = pl.program_id(0)
    copies = [pltpu.make_async_copy(src, dst, sems.at[index]) for index, (src, dst) in enumerate(
        ((w_out_hbm, w_out), (w_up_hbm, w_up), (w_down_hbm, w_down), (wk_hbm, wk), (wv_hbm, wv)))]

    @pl.when(step == 0)
    def _():
        for copy in copies:
            copy.start()
        pooled_ref[...] = jnp.zeros_like(pooled_ref)
        total_ref[...] = jnp.zeros_like(total_ref)
        peak_ref[...] = jnp.full_like(peak_ref, -jnp.inf)

    def arrive(index):
        @pl.when(step == 0)
        def _():
            copies[index].wait()

    b_out, ln2_gain, ln2_bias, b_down, lnf_gain, lnf_bias = (vec_ref[index:index + 1, :] for index in range(6))
    arrive(0)
    attn_local = jnp.dot(mixed_ref[...], w_out[...], preferred_element_type=jnp.float32)
    resid_one = (resid_ref[...].astype(jnp.float32) + attn_local + b_out).astype(jnp.bfloat16)
    hidden_two = layer_norm(resid_one.astype(jnp.float32), ln2_gain, ln2_bias).astype(jnp.bfloat16)
    arrive(1)
    n_units = w_up.shape[0]
    for start in range(0, n_units, up_chunk):
        cols = slice(start, min(start + up_chunk, n_units))
        pre_act = lax.dot_general(hidden_two, w_up[cols, :], (((1,), (1,)), ((), ())), preferred_element_type=jnp.float32) + up_bias_ref[:, cols]
        units[:, cols] = jax.nn.gelu(pre_act, approximate=True).astype(jnp.bfloat16)
    arrive(2)
    mlp_local = jnp.dot(units[...], w_down[...], preferred_element_type=jnp.float32)
    resid_two = (resid_one.astype(jnp.float32) + mlp_local + b_down).astype(jnp.bfloat16)
    encoded = layer_norm(resid_two.astype(jnp.float32), lnf_gain, lnf_bias).astype(jnp.bfloat16)
    arrive(3)
    keys = (jnp.dot(encoded, wk[...], preferred_element_type=jnp.float32) + pool_bias_ref[0:1, :]).astype(jnp.bfloat16)
    arrive(4)
    values = (jnp.dot(encoded, wv[...], preferred_element_type=jnp.float32) + pool_bias_ref[1:2, :]).astype(jnp.bfloat16)
    scores = lax.dot_general(probe_ref[...], keys, (((1,), (1,)), ((), ())), preferred_element_type=jnp.float32) * head_dim ** -0.5
    peak = jnp.maximum(peak_ref[...], jnp.max(scores, axis=-1, keepdims=True))
    weights = jnp.exp(scores - peak)
    keep = jnp.exp(peak_ref[...] - peak)
    total_ref[...] = total_ref[...] * keep + jnp.sum(weights, axis=-1, keepdims=True)
    pooled_ref[...] = pooled_ref[...] * keep + jnp.dot(weights.astype(jnp.bfloat16), values, preferred_element_type=jnp.float32)
    peak_ref[...] = peak


def finish_tokens(mixed, resid, vectors, up_bias, pool_bias, probe, weights, head_dim, block=512):
    n_own, width = resid.shape
    n_heads = probe.shape[0]
    n_units = up_bias.shape[1]
    fixed = lambda shape: pl.BlockSpec(shape, lambda i: (0, 0))
    small = [vectors, up_bias, pool_bias, probe]
    return pl.pallas_call(
        functools.partial(finish_kernel, head_dim, 512),
        grid=(n_own // block,),
        out_shape=[jax.ShapeDtypeStruct((n_heads, columns), jnp.float32) for columns in (width, 1, 1)],
        in_specs=[pl.BlockSpec((block, mixed.shape[1]), lambda i: (i, 0)), pl.BlockSpec((block, width), lambda i: (i, 0))]
        + [fixed(array.shape) for array in small] + [pl.BlockSpec(memory_space=pl.ANY)] * len(weights),
        out_specs=[fixed((n_heads, columns)) for columns in (width, 1, 1)],
        scratch_shapes=[pltpu.VMEM(weight.shape, jnp.bfloat16) for weight in weights]
        + [pltpu.VMEM((block, n_units), jnp.bfloat16), pltpu.SemaphoreType.DMA((len(weights),))],
        compiler_params=pltpu.CompilerParams(dimension_semantics=('arbitrary',), vmem_limit_bytes=60 * 1024 * 1024),
        cost_estimate=pl.CostEstimate(flops=2 * n_own * sum(weight.size for weight in weights), bytes_accessed=40 * 1024 * 1024, transcendentals=n_own * n_units),
        name='finish_tokens',
    )(mixed, resid, *small, *weights)


def map_tail(pooled_heads, map_wo, map_bo, map_ln_gain, map_ln_bias, map_w_up, map_b_up, map_w_down, map_b_down):
    attn_vec = jnp.einsum('bhe,hed->bd', pooled_heads, map_wo, preferred_element_type=jnp.float32) + map_bo
    map_hidden = layer_norm(attn_vec, map_ln_gain, map_ln_bias).astype(jnp.bfloat16)
    map_act = jax.nn.gelu(jnp.dot(map_hidden, map_w_up, preferred_element_type=jnp.float32) + map_b_up, approximate=True).astype(jnp.bfloat16)
    return (attn_vec + jnp.dot(map_act, map_w_down, preferred_element_type=jnp.float32) + map_b_down).astype(jnp.bfloat16)


def solution(mesh):
    tp_size = mesh.shape['tp']
    in_specs = (P('dp', 'tp', None), P(), P(), P(None, None, 'tp', None), P(None, 'tp', None), P('tp', None, None), P(), P(), P(), P(None, 'tp'), P('tp'), P('tp', None)) + (P(),) * 16
    partner = [(device, device ^ 1) for device in range(tp_size)]

    def local_program(tokens, ln1_gain, ln1_bias, w_qkv, b_qkv, w_out, b_out, ln2_gain, ln2_bias, w_up, b_up, w_down, b_down, lnf_gain, lnf_bias, probe_vec, map_wq, map_bq, map_wkv, map_bkv, map_wo, map_bo, map_ln_gain, map_ln_bias, map_w_up, map_b_up, map_w_down, map_b_down):
        n_images, run, width = tokens.shape
        groups, head_dim = w_qkv.shape[2:]
        n_heads = groups * tp_size
        hidden_units = w_up.shape[1]
        own = n_images * run

        resid = row_major(lax.all_to_all(row_major(tokens.reshape(tp_size, own // tp_size, width)), 'tp', split_axis=0, concat_axis=0, tiled=True).reshape(own, width))

        rows_padded = round_up(head_dim, 16)
        shards = []
        for group in range(groups):
            rows = jnp.transpose(w_qkv[:, :, group], (1, 2, 0))
            bias_row = jnp.concatenate(split_three(b_qkv[:, group].reshape(3 * head_dim)))
            bias_row = jnp.pad(bias_row, (0, width - bias_row.shape[0]))[None]
            extra = jnp.pad(bias_row, ((0, rows_padded - head_dim - 1), (0, 0)))
            none = jnp.zeros_like(extra)
            shards.append(jnp.concatenate([rows[0], none, rows[1], none, rows[2], extra], axis=0))
        padded = round_up(hidden_units, 32)
        w_up_t = jnp.pad(w_up.T, ((0, padded - hidden_units), (0, 0)))
        high, middle, low = split_three(b_up)
        up_rows = jnp.stack([jnp.pad(jnp.concatenate([high, middle]), (0, width - 2 * hidden_units)), jnp.pad(low, (0, width - hidden_units))])
        w_down_p = jnp.pad(jnp.concatenate([w_down, up_rows], axis=0), ((0, padded - hidden_units - 2), (0, 0)))

        gathered = [lax.all_gather(shards[0], 'tp', axis=0, tiled=True)]
        probe_q = (jnp.dot(probe_vec[None], map_wq.reshape(width, width), preferred_element_type=jnp.float32)[0] + map_bq.reshape(width)).astype(jnp.bfloat16)
        head_of = jnp.arange(width) // head_dim
        on_head = head_of[:, None] == jnp.arange(n_heads)[None]
        probe_cols = jnp.where(on_head.T, probe_q[None], jnp.zeros((), jnp.bfloat16))
        pool_wk, pool_wv = (row_major(map_wkv[:, index].reshape(width, width)) for index in range(2))
        vectors = jnp.stack([b_out, ln2_gain, ln2_bias, b_down, lnf_gain, lnf_bias])
        w_out_p = jnp.pad(w_out, ((0, 0), (0, LANES - head_dim), (0, 0))).reshape(groups * LANES, width)
        resid, later, w_out_p, w_up_t, w_down_p, probe_cols, pool_wk, pool_wv, vectors, pool_bias = lax.optimization_barrier(
            (resid, shards[1:], w_out_p, w_up_t, w_down_p, probe_cols, pool_wk, pool_wv, vectors, map_bkv.reshape(2, width)))
        gathered += [lax.all_gather(shard, 'tp', axis=0, tiled=True) for shard in later]
        w_out_all = lax.all_gather(w_out_p, 'tp', axis=0, tiled=True)
        w_up_all = lax.all_gather(w_up_t, 'tp', axis=0, tiled=True)
        w_down_all = lax.all_gather(w_down_p, 'tp', axis=0, tiled=True)

        def projections(group_rows, resid):
            bias_row = group_rows.reshape(tp_size, 3 * rows_padded, width)[:, 2 * rows_padded + head_dim, :9 * head_dim]
            bias_row = bias_row.reshape(tp_size, 3, 3, head_dim)
            bias = join_three([bias_row[:, term] for term in range(3)])
            bias = jnp.pad(bias, ((0, 0), (0, 0), (0, rows_padded - head_dim))).reshape(-1, 1)
            first = project_tokens(resid, 0, ln1_gain, ln1_bias, group_rows, bias)
            second = project_tokens(resid, 1, ln1_gain, ln1_bias, group_rows, bias)
            return [first, second, lax.ppermute(first, 'tp', partner), lax.ppermute(second, 'tp', partner)]

        half = tp_size // 2
        first_group = projections(gathered[0], resid)
        mixed = heads_attention(first_group, head_dim, (0, half), 0, groups, None, n_heads)
        mixed, resid, gathered[1] = lax.optimization_barrier((mixed, resid, gathered[1]))
        second_group = projections(gathered[1], resid)
        mixed = heads_attention(first_group, head_dim, (half, half), 0, groups, mixed, n_heads)
        mixed = heads_attention(second_group, head_dim, (0, tp_size), 1, groups, mixed, n_heads)

        bias_rows = w_down_all.reshape(tp_size, padded, width)[:, hidden_units:hidden_units + 2]
        b_up_all = join_three([bias_rows[:, 0, :hidden_units], bias_rows[:, 0, hidden_units:2 * hidden_units], bias_rows[:, 1, :hidden_units]])
        b_up_all = jnp.pad(b_up_all, ((0, 0), (0, padded - hidden_units))).reshape(tp_size * padded)
        every_head, total, peak = finish_tokens(
            mixed.reshape(own, n_heads * LANES), resid, vectors, b_up_all[None], pool_bias, probe_cols, (w_out_all, w_up_all, w_down_all, pool_wk, pool_wv), head_dim)
        pooled = jnp.sum(jnp.where(on_head.T, every_head, 0.0).reshape(n_heads, n_heads, head_dim), axis=1)
        parts = lax.all_gather(jnp.concatenate([pooled, total, peak], axis=-1), 'tp', axis=0, tiled=False)
        parts = parts.reshape(n_images, tp_size // n_images, n_heads, head_dim + 2)
        pooled_all, total_all, peak_all = parts[..., :head_dim], parts[..., head_dim:head_dim + 1], parts[..., head_dim + 1:]
        share = jnp.exp(peak_all - jnp.max(peak_all, axis=1, keepdims=True))
        pooled_heads = (jnp.sum(pooled_all * share, axis=1) / jnp.sum(total_all * share, axis=1)).astype(jnp.bfloat16)
        return map_tail(pooled_heads, map_wo, map_bo, map_ln_gain, map_ln_bias, map_w_up, map_b_up, map_w_down, map_b_down)

    return jax.shard_map(local_program, mesh=mesh, in_specs=in_specs, out_specs=P('dp', None), check_vma=False)
```

```python
import functools

import jax
import jax.numpy as jnp
from jax import lax
from jax.experimental import pallas as pl
from jax.experimental.layout import Layout, with_layout_constraint
from jax.experimental.pallas import tpu as pltpu
from jax.sharding import PartitionSpec as P

LN_EPS = 1e-6
LOG2E = 1.4426950408889634
LANES = 128
BF16_MAX = 3.3895313892515355e38


def layer_norm(values, gain_vec, bias_vec):
    centered = values - jnp.mean(values, axis=-1, keepdims=True)
    variance = jnp.mean(centered * centered, axis=-1, keepdims=True)
    return centered * lax.rsqrt(variance + LN_EPS) * gain_vec + bias_vec


def row_major(values):
    return with_layout_constraint(values, Layout(major_to_minor=tuple(range(values.ndim))))


def round_up(size, multiple):
    return -(-size // multiple) * multiple


def attention_kernel(head_dim, chunk, *refs):
    out_ref, scores_a, scores_b, max_a, max_b, first_out, apart = refs[-7:]
    q_refs, k_refs, v_refs, v_last_refs = refs[:2], refs[2:6], refs[6:10], refs[10:14]
    part_keys = k_refs[0].shape[1]
    block = q_refs[0].shape[1]
    step = pl.program_id(0)
    exp_scale = head_dim ** -0.5 * LOG2E

    def score_chunk(keys_t, queries, rows, scores, running):
        part = lax.dot_general(keys_t, queries, (((0,), (0,)), ((), ())), preferred_element_type=jnp.float32)
        scores[rows, :] = part
        part_max = jnp.max(part.reshape(chunk // 8, 8, block), axis=0)
        return part_max if running is None else jnp.maximum(running, part_max)

    def mix_chunk(values, rows, scores, peak, total, mixed):
        weights = jnp.exp2((scores[rows, :] - peak) * exp_scale)
        part_total = jnp.sum(weights.reshape(chunk // 8, 8, block), axis=0)
        part_mixed = jnp.dot(values, weights.astype(jnp.bfloat16), preferred_element_type=jnp.float32)
        if total is None:
            return part_total, part_mixed
        return total + part_total, mixed + part_mixed

    def overlap(query_slot, score_buf, max_buf, v_parts, mix_buf, mix_max):
        running, total, mixed = None, None, None
        peak = jnp.max(mix_max[...], axis=0, keepdims=True)
        queries = q_refs[query_slot][...]
        for part, (k_ref, v_ref) in enumerate(zip(k_refs, v_parts)):
            for start in range(0, part_keys, chunk):
                rows = pl.ds(part * part_keys + start, chunk)
                running = score_chunk(k_ref[:, start:start + chunk], queries, rows, score_buf, running)
                total, mixed = mix_chunk(v_ref[:, start:start + chunk], rows, mix_buf, peak, total, mixed)
        max_buf[...] = running
        return mixed[:head_dim] / jnp.sum(total, axis=0, keepdims=True)

    def write(half, values_t):
        filled = jnp.concatenate([values_t, jnp.zeros((LANES - head_dim, block), jnp.float32)], axis=0)
        out_ref[half] = filled.T.astype(out_ref.dtype)

    @pl.when(step == 0)
    def _():
        apart[0] = 0
        max_b[...] = jnp.zeros_like(max_b)
        first_out[...] = jnp.zeros_like(first_out)

    @pl.when(apart[0] == 0)
    def _():
        second = overlap(0, scores_a, max_a, v_last_refs, scores_b, max_b)
        write(0, first_out[...])
        write(1, second)

    @pl.when(step < pl.num_programs(0) - 1)
    def _():
        first_out[...] = overlap(1, scores_b, max_b, v_refs, scores_a, max_a)


def heads_attention(parts, head_dim, heads, place, stride, previous, n_out):
    first, count = heads
    n_part = parts[0].shape[1]
    block = n_part // 2
    per_head = n_part // block
    last = count * per_head - 1
    now = lambda i: first + jnp.minimum(i, last) // per_head
    before = lambda i: first + jnp.maximum(i - 1, 0) // per_head
    rows = round_up(head_dim, 16)
    whole = (rows, n_part)
    in_specs = [pl.BlockSpec((rows, block), lambda i: (3 * now(i), jnp.minimum(i, last) % per_head))] * 2
    in_specs += [pl.BlockSpec(whole, lambda i: (3 * now(i) + 1, 0))] * 4
    in_specs += [pl.BlockSpec(whole, lambda i: (3 * now(i) + 2, 0))] * 4
    in_specs += [pl.BlockSpec(whole, lambda i: (3 * before(i) + 2, 0))] * 4
    operands = [*parts[:2], *parts, *parts, *parts]
    aliases = {}
    if previous is not None:
        in_specs.append(pl.BlockSpec(memory_space=pl.ANY))
        operands.append(previous)
        aliases = {len(operands) - 1: 0}
    scored = count * 2 * n_part * 4 * n_part
    return pl.pallas_call(
        functools.partial(attention_kernel, head_dim, 256),
        grid=(last + 2,),
        out_shape=jax.ShapeDtypeStruct((2, n_part, n_out * LANES), jnp.bfloat16),
        in_specs=in_specs,
        out_specs=pl.BlockSpec((2, block, LANES), lambda i: (0, jnp.maximum(i - 1, 0) % per_head, place + stride * before(i))),
        scratch_shapes=[
            pltpu.VMEM((4 * n_part, block), jnp.float32),
            pltpu.VMEM((4 * n_part, block), jnp.float32),
            pltpu.VMEM((8, block), jnp.float32),
            pltpu.VMEM((8, block), jnp.float32),
            pltpu.VMEM((head_dim, block), jnp.float32),
            pltpu.SMEM((1,), jnp.int32),
        ],
        input_output_aliases=aliases,
        compiler_params=pltpu.CompilerParams(dimension_semantics=('arbitrary',), vmem_limit_bytes=60 * 1024 * 1024),
        cost_estimate=pl.CostEstimate(flops=4 * scored * LANES, bytes_accessed=8 * 1024 * 1024, transcendentals=scored),
        name='heads_attention',
    )(*operands)


def project_kernel(per_out, x_ref, gain_ref, shift_ref, weight_ref, bias_ref, *out_refs):
    hidden = layer_norm(x_ref[...].astype(jnp.float32), gain_ref[...], shift_ref[...]).astype(jnp.bfloat16)
    product = lax.dot_general(weight_ref[...], hidden, (((1,), (1,)), ((), ())), preferred_element_type=jnp.float32)
    for index, out_ref in enumerate(out_refs):
        @pl.when(pl.program_id(0) // per_out == index)
        def _():
            out_ref[...] = (product + bias_ref[...]).astype(out_ref.dtype)


def project_tokens(resid, parts, gain, shift, weight, bias, block=512):
    n_own, width = resid.shape[0] // 2, resid.shape[1]
    per_out = n_own // block
    first = parts[0] * per_out
    out_spec = lambda index: pl.BlockSpec((rows, block), lambda i: (0, jnp.clip(i - index * per_out, 0, per_out - 1)))
    rows = weight.shape[0]
    fixed = lambda shape: pl.BlockSpec(shape, lambda i: (0, 0))
    return pl.pallas_call(
        functools.partial(project_kernel, per_out),
        grid=(len(parts) * per_out,),
        out_shape=[jax.ShapeDtypeStruct((rows, n_own), jnp.bfloat16)] * len(parts),
        in_specs=[pl.BlockSpec((block, width), lambda i: (first + i, 0)), fixed((1, width)), fixed((1, width)), fixed((rows, width)), fixed((rows, 1))],
        out_specs=[out_spec(index) for index in range(len(parts))],
        compiler_params=pltpu.CompilerParams(dimension_semantics=('arbitrary',), vmem_limit_bytes=60 * 1024 * 1024),
        cost_estimate=pl.CostEstimate(flops=2 * n_own * width * rows, bytes_accessed=2 * (n_own * width + rows * width + rows * n_own), transcendentals=n_own),
        name='project_tokens',
    )(resid, gain[None], shift[None], weight, bias)


def split_three(values):
    high = lax.reduce_precision(jnp.clip(values, -BF16_MAX, BF16_MAX), 8, 7)
    middle = lax.reduce_precision(values - high, 8, 7)
    return [high.astype(jnp.bfloat16), middle.astype(jnp.bfloat16), (values - high - middle).astype(jnp.bfloat16)]


def join_three(parts):
    high, middle, low = (part.astype(jnp.float32) for part in parts)
    return high + middle + low


def finish_kernel(head_dim, up_chunk, mixed_ref, resid_ref, vec_ref, up_bias_ref, pool_bias_ref, probe_ref, w_out_hbm, w_up_hbm, w_down_hbm, wk_hbm, wv_hbm,
                  pooled_ref, total_ref, peak_ref, w_out, w_up, w_down, wk, wv, units, sems):
    step = pl.program_id(0)
    copies = [pltpu.make_async_copy(src, dst, sems.at[index]) for index, (src, dst) in enumerate(
        ((w_out_hbm, w_out), (w_up_hbm, w_up), (w_down_hbm, w_down), (wk_hbm, wk), (wv_hbm, wv)))]

    @pl.when(step == 0)
    def _():
        for copy in copies:
            copy.start()
        pooled_ref[...] = jnp.zeros_like(pooled_ref)
        total_ref[...] = jnp.zeros_like(total_ref)
        peak_ref[...] = jnp.full_like(peak_ref, -jnp.inf)

    def arrive(index):
        @pl.when(step == 0)
        def _():
            copies[index].wait()

    b_out, ln2_gain, ln2_bias, b_down, lnf_gain, lnf_bias = (vec_ref[index:index + 1, :] for index in range(6))
    arrive(0)
    attn_local = jnp.dot(mixed_ref[...], w_out[...], preferred_element_type=jnp.float32)
    resid_one = (resid_ref[...].astype(jnp.float32) + attn_local + b_out).astype(jnp.bfloat16)
    hidden_two = layer_norm(resid_one.astype(jnp.float32), ln2_gain, ln2_bias).astype(jnp.bfloat16)
    arrive(1)
    n_units = w_up.shape[0]
    for start in range(0, n_units, up_chunk):
        cols = slice(start, min(start + up_chunk, n_units))
        pre_act = lax.dot_general(hidden_two, w_up[cols, :], (((1,), (1,)), ((), ())), preferred_element_type=jnp.float32) + up_bias_ref[:, cols]
        units[:, cols] = jax.nn.gelu(pre_act, approximate=True).astype(jnp.bfloat16)
    arrive(2)
    mlp_local = jnp.dot(units[...], w_down[...], preferred_element_type=jnp.float32)
    resid_two = (resid_one.astype(jnp.float32) + mlp_local + b_down).astype(jnp.bfloat16)
    encoded = layer_norm(resid_two.astype(jnp.float32), lnf_gain, lnf_bias).astype(jnp.bfloat16)
    arrive(3)
    keys = (jnp.dot(encoded, wk[...], preferred_element_type=jnp.float32) + pool_bias_ref[0:1, :]).astype(jnp.bfloat16)
    arrive(4)
    values = (jnp.dot(encoded, wv[...], preferred_element_type=jnp.float32) + pool_bias_ref[1:2, :]).astype(jnp.bfloat16)
    scores = lax.dot_general(probe_ref[...], keys, (((1,), (1,)), ((), ())), preferred_element_type=jnp.float32) * head_dim ** -0.5
    peak = jnp.maximum(peak_ref[...], jnp.max(scores, axis=-1, keepdims=True))
    weights = jnp.exp(scores - peak)
    keep = jnp.exp(peak_ref[...] - peak)
    total_ref[...] = total_ref[...] * keep + jnp.sum(weights, axis=-1, keepdims=True)
    pooled_ref[...] = pooled_ref[...] * keep + jnp.dot(weights.astype(jnp.bfloat16), values, preferred_element_type=jnp.float32)
    peak_ref[...] = peak


def finish_tokens(mixed, resid, vectors, up_bias, pool_bias, probe, weights, head_dim, block=512):
    n_own, width = resid.shape
    n_heads = probe.shape[0]
    n_units = up_bias.shape[1]
    fixed = lambda shape: pl.BlockSpec(shape, lambda i: (0, 0))
    small = [vectors, up_bias, pool_bias, probe]
    return pl.pallas_call(
        functools.partial(finish_kernel, head_dim, 512),
        grid=(n_own // block,),
        out_shape=[jax.ShapeDtypeStruct((n_heads, columns), jnp.float32) for columns in (width, 1, 1)],
        in_specs=[pl.BlockSpec((block, mixed.shape[1]), lambda i: (i, 0)), pl.BlockSpec((block, width), lambda i: (i, 0))]
        + [fixed(array.shape) for array in small] + [pl.BlockSpec(memory_space=pl.ANY)] * len(weights),
        out_specs=[fixed((n_heads, columns)) for columns in (width, 1, 1)],
        scratch_shapes=[pltpu.VMEM(weight.shape, jnp.bfloat16) for weight in weights]
        + [pltpu.VMEM((block, n_units), jnp.bfloat16), pltpu.SemaphoreType.DMA((len(weights),))],
        compiler_params=pltpu.CompilerParams(dimension_semantics=('arbitrary',), vmem_limit_bytes=60 * 1024 * 1024),
        cost_estimate=pl.CostEstimate(flops=2 * n_own * sum(weight.size for weight in weights), bytes_accessed=40 * 1024 * 1024, transcendentals=n_own * n_units),
        name='finish_tokens',
    )(mixed, resid, *small, *weights)


def map_tail(pooled_heads, map_wo, map_bo, map_ln_gain, map_ln_bias, map_w_up, map_b_up, map_w_down, map_b_down):
    attn_vec = jnp.einsum('bhe,hed->bd', pooled_heads, map_wo, preferred_element_type=jnp.float32) + map_bo
    map_hidden = layer_norm(attn_vec, map_ln_gain, map_ln_bias).astype(jnp.bfloat16)
    map_act = jax.nn.gelu(jnp.dot(map_hidden, map_w_up, preferred_element_type=jnp.float32) + map_b_up, approximate=True).astype(jnp.bfloat16)
    return (attn_vec + jnp.dot(map_act, map_w_down, preferred_element_type=jnp.float32) + map_b_down).astype(jnp.bfloat16)


def solution(mesh):
    tp_size = mesh.shape['tp']
    in_specs = (P('dp', 'tp', None), P(), P(), P(None, None, 'tp', None), P(None, 'tp', None), P('tp', None, None), P(), P(), P(), P(None, 'tp'), P('tp'), P('tp', None)) + (P(),) * 16
    partner = [(device, device ^ 1) for device in range(tp_size)]

    def local_program(tokens, ln1_gain, ln1_bias, w_qkv, b_qkv, w_out, b_out, ln2_gain, ln2_bias, w_up, b_up, w_down, b_down, lnf_gain, lnf_bias, probe_vec, map_wq, map_bq, map_wkv, map_bkv, map_wo, map_bo, map_ln_gain, map_ln_bias, map_w_up, map_b_up, map_w_down, map_b_down):
        n_images, run, width = tokens.shape
        groups, head_dim = w_qkv.shape[2:]
        n_heads = groups * tp_size
        hidden_units = w_up.shape[1]
        own = n_images * run

        resid = row_major(lax.all_to_all(row_major(tokens.reshape(tp_size, own // tp_size, width)), 'tp', split_axis=0, concat_axis=0, tiled=True).reshape(own, width))

        rows_padded = round_up(head_dim, 16)
        shards = []
        for group in range(groups):
            rows = jnp.transpose(w_qkv[:, :, group], (1, 2, 0))
            bias_row = jnp.concatenate(split_three(b_qkv[:, group].reshape(3 * head_dim)))
            bias_row = jnp.pad(bias_row, (0, width - bias_row.shape[0]))[None]
            extra = jnp.pad(bias_row, ((0, rows_padded - head_dim - 1), (0, 0)))
            none = jnp.zeros_like(extra)
            shards.append(jnp.concatenate([rows[0], none, rows[1], none, rows[2], extra], axis=0))
        padded = round_up(hidden_units, 32)
        w_up_t = jnp.pad(w_up.T, ((0, padded - hidden_units), (0, 0)))
        high, middle, low = split_three(b_up)
        up_rows = jnp.stack([jnp.pad(jnp.concatenate([high, middle]), (0, width - 2 * hidden_units)), jnp.pad(low, (0, width - hidden_units))])
        w_down_p = jnp.pad(jnp.concatenate([w_down, up_rows], axis=0), ((0, padded - hidden_units - 2), (0, 0)))

        gathered = [lax.all_gather(shards[0], 'tp', axis=0, tiled=True)]
        probe_q = (jnp.dot(probe_vec[None], map_wq.reshape(width, width), preferred_element_type=jnp.float32)[0] + map_bq.reshape(width)).astype(jnp.bfloat16)
        head_of = jnp.arange(width) // head_dim
        on_head = head_of[:, None] == jnp.arange(n_heads)[None]
        probe_cols = jnp.where(on_head.T, probe_q[None], jnp.zeros((), jnp.bfloat16))
        pool_wk, pool_wv = (row_major(map_wkv[:, index].reshape(width, width)) for index in range(2))
        vectors = jnp.stack([b_out, ln2_gain, ln2_bias, b_down, lnf_gain, lnf_bias])
        w_out_p = jnp.pad(w_out, ((0, 0), (0, LANES - head_dim), (0, 0))).reshape(groups * LANES, width)
        resid, later, w_out_p, w_up_t, w_down_p, probe_cols, pool_wk, pool_wv, vectors, pool_bias = lax.optimization_barrier(
            (resid, shards[1:], w_out_p, w_up_t, w_down_p, probe_cols, pool_wk, pool_wv, vectors, map_bkv.reshape(2, width)))
        gathered += [lax.all_gather(shard, 'tp', axis=0, tiled=True) for shard in later]
        w_out_all = lax.all_gather(w_out_p, 'tp', axis=0, tiled=True)
        w_up_all = lax.all_gather(w_up_t, 'tp', axis=0, tiled=True)
        w_down_all = lax.all_gather(w_down_p, 'tp', axis=0, tiled=True)

        def projections(group_rows, resid, calls):
            bias_row = group_rows.reshape(tp_size, 3 * rows_padded, width)[:, 2 * rows_padded + head_dim, :9 * head_dim]
            bias_row = bias_row.reshape(tp_size, 3, 3, head_dim)
            bias = join_three([bias_row[:, term] for term in range(3)])
            bias = jnp.pad(bias, ((0, 0), (0, 0), (0, rows_padded - head_dim))).reshape(-1, 1)
            first, second = (part for parts in calls for part in project_tokens(resid, parts, ln1_gain, ln1_bias, group_rows, bias))
            return [first, second, lax.ppermute(first, 'tp', partner), lax.ppermute(second, 'tp', partner)]

        half = tp_size // 2
        first_group = projections(gathered[0], resid, [(0,), (1,)])
        mixed = heads_attention(first_group, head_dim, (0, half), 0, groups, None, n_heads)
        mixed, resid, gathered[1] = lax.optimization_barrier((mixed, resid, gathered[1]))
        second_group = projections(gathered[1], resid, [(0, 1)])
        mixed = heads_attention(first_group, head_dim, (half, half), 0, groups, mixed, n_heads)
        mixed = heads_attention(second_group, head_dim, (0, tp_size), 1, groups, mixed, n_heads)

        bias_rows = w_down_all.reshape(tp_size, padded, width)[:, hidden_units:hidden_units + 2]
        b_up_all = join_three([bias_rows[:, 0, :hidden_units], bias_rows[:, 0, hidden_units:2 * hidden_units], bias_rows[:, 1, :hidden_units]])
        b_up_all = jnp.pad(b_up_all, ((0, 0), (0, padded - hidden_units))).reshape(tp_size * padded)
        every_head, total, peak = finish_tokens(
            mixed.reshape(own, n_heads * LANES), resid, vectors, b_up_all[None], pool_bias, probe_cols, (w_out_all, w_up_all, w_down_all, pool_wk, pool_wv), head_dim)
        pooled = jnp.sum(jnp.where(on_head.T, every_head, 0.0).reshape(n_heads, n_heads, head_dim), axis=1)
        parts = lax.all_gather(jnp.concatenate([pooled, total, peak], axis=-1), 'tp', axis=0, tiled=False)
        parts = parts.reshape(n_images, tp_size // n_images, n_heads, head_dim + 2)
        pooled_all, total_all, peak_all = parts[..., :head_dim], parts[..., head_dim:head_dim + 1], parts[..., head_dim + 1:]
        share = jnp.exp(peak_all - jnp.max(peak_all, axis=1, keepdims=True))
        pooled_heads = (jnp.sum(pooled_all * share, axis=1) / jnp.sum(total_all * share, axis=1)).astype(jnp.bfloat16)
        return map_tail(pooled_heads, map_wo, map_bo, map_ln_gain, map_ln_bias, map_w_up, map_b_up, map_w_down, map_b_down)

    return jax.shard_map(local_program, mesh=mesh, in_specs=in_specs, out_specs=P('dp', None), check_vma=False)
```
